32 devices in a mesh: tm: 4 (over x, core), space: 8 (over z, y).
Axes of the slice: x: 2, y: 2, z: 4, core: 2. Of those that a mesh axis runs over, the one named last changes fastest.
Arguments:
- iterate: float32 [64, 16, 3, 4096], P('space', 'tm'), may hold values from -6 to 6
- forcing: float32 [64, 16, 3, 4096], P('space', 'tm'), may hold values from -6 to 6
- initial_velocity: float32 [64, 3, 4096], P('space'), may hold values from -6 to 6
- viscosity: float32 [64, 4096], P('space'), may hold values from 0.1 to 1
- peclet: float32 [64, 3, 4096], P('space'), may hold values from -0.9 to 0.9
- live_patch_mask: int32 [64], P('space'), may hold values from 0 to 1, as said below
- neighbour_holder: int32 [64, 6], P('space'), may hold values from -1 to 7, as said below
- neighbour_slot: int32 [64, 6], P('space'), may hold values from -1 to 7, as said below
Outputs:
- corrected_velocity: float32 [64, 16, 3, 4096], P('space', 'tm')
- corrected_residual: float32 [64, 16, 3, 4096], P('space', 'tm')
The draws below stay inside these ranges and needn't reach their ends.
Inputs may be any that keep to these rules, and one draw needn't show every extreme that they name: `live_patch_mask`: on each index of space the live slots (1) come first; their count is 2 to 8, and in every draw some two indices j and j + 4 have all 8 slots live. `neighbour_holder`: the patches of one index s of space are the blocks of one aligned 2x2x2 octant; the octant's position is read from the bits of s: bit b of s is bit b div 3 of coordinate b mod 3, except that where a coordinate has two bits its lower bit is complemented when its higher bit is 1; slot p lies at offsets (p mod 2, p div 2 mod 2, p div 4); the entry is -1 where no live patch lies across the face or the slot is dead; the relation is symmetric across opposite faces; the live patches of one index face those of another given index across at most 4 faces, exactly 4 for some pair in every draw. `neighbour_slot`: -1 exactly where neighbour_holder is -1.
All inputs are finite; a program needn't handle non-finite values.
Results may differ from the reference program's by a relative error of at most 0.0003.
Values sent between devices are 32-bit elements; how exact they have to be, the bound alone decides.
No kernel may reach another device: no remote copies, remote signals or barrier semaphores. Data moves between devices by JAX's collectives and lax.ppermute only.
A program may use at most 192 MiB of HBM per device.

```python
import math
from functools import partial
import jax
import jax.numpy as jnp
from jax import lax

WINDOW_SLICES = 16
BLOCK_EDGE = 16
SLOTS_PER_SPACE = 8
SWEEPS = 5
TOTAL_SLOTS = 64
BLOCK_CELLS = 4096


def octant_layout(key):
    key = jax.random.fold_in(key, 7919)
    count_key, pair_key = jax.random.split(key)
    space_members = TOTAL_SLOTS // SLOTS_PER_SPACE
    levels = max(space_members - 1, 1).bit_length()
    half_members = max(space_members // 2, 1)
    counts = jax.random.randint(count_key, (space_members,), 2, 7)
    chosen = jax.random.randint(pair_key, (), 0, half_members)
    if space_members >= 16:
        chosen = jnp.bitwise_or(chosen, 1)
    device_ids = jnp.arange(space_members, dtype=jnp.int32)
    counts = jnp.where(device_ids % half_members == chosen, SLOTS_PER_SPACE, counts).astype(jnp.int32)
    slot_numbers = jnp.arange(TOTAL_SLOTS, dtype=jnp.int32)
    holders = slot_numbers // SLOTS_PER_SPACE
    local_slot = slot_numbers % SLOTS_PER_SPACE
    octant = [jnp.zeros_like(slot_numbers), jnp.zeros_like(slot_numbers), jnp.zeros_like(slot_numbers)]
    extents = [2, 2, 2]
    coord_bits = [0, 0, 0]
    for bit_index in range(levels):
        octant[bit_index % 3] = octant[bit_index % 3] + ((holders >> bit_index & 1) << bit_index // 3)
        extents[bit_index % 3] = extents[bit_index % 3] * 2
        coord_bits[bit_index % 3] = coord_bits[bit_index % 3] + 1
    for axis_id in range(3):
        if coord_bits[axis_id] == 2:
            octant[axis_id] = jnp.bitwise_xor(octant[axis_id], octant[axis_id] >> 1 & 1)
    coords = [2 * octant[axis_id] + (local_slot >> axis_id & 1) for axis_id in range(3)]
    live_self = local_slot < counts[holders]
    owner_columns = []
    slot_columns = []
    for face_id in range(6):
        axis_id = face_id // 2
        shifted = list(coords)
        shifted[axis_id] = coords[axis_id] + (2 * (face_id % 2) - 1)
        inside = (shifted[axis_id] >= 0) & (shifted[axis_id] < extents[axis_id])
        clipped = [jnp.clip(shifted[other_axis], 0, extents[other_axis] - 1) for other_axis in range(3)]
        decoded = []
        for other_axis in range(3):
            value = clipped[other_axis] // 2
            if coord_bits[other_axis] == 2:
                value = jnp.bitwise_xor(value, value >> 1 & 1)
            decoded.append(value)
        octant_code = jnp.zeros_like(slot_numbers)
        for bit_index in range(levels):
            octant_code = octant_code + ((decoded[bit_index % 3] >> bit_index // 3 & 1) << bit_index)
        neighbour_local = (clipped[0] & 1) + ((clipped[1] & 1) << 1) + ((clipped[2] & 1) << 2)
        in_range = octant_code < space_members
        safe_code = jnp.minimum(octant_code, space_members - 1)
        present = inside & in_range & live_self & (neighbour_local < counts[safe_code])
        owner_columns.append(jnp.where(present, octant_code, -1))
        slot_columns.append(jnp.where(present, neighbour_local, -1))
    live_mask = live_self.astype(jnp.int32)
    return (live_mask, jnp.stack(owner_columns, axis=1).astype(jnp.int32), jnp.stack(slot_columns, axis=1).astype(jnp.int32))


def draw_live_patch_mask(key, part):
    return octant_layout(key)[0]


def draw_neighbour_holder(key, part):
    return octant_layout(key)[1]


def draw_neighbour_slot(key, part):
    return octant_layout(key)[2]


def steps_of(rng, shape, cuts, low, largest):
    level = 1.0
    for dim, parts in cuts:
        draws = jax.random.uniform(jax.random.fold_in(jax.random.fold_in(rng, 6), dim), (parts,), jnp.float32, low / len(cuts), largest / len(cuts))
        level = level * jnp.repeat(jnp.exp(draws), shape[dim] // parts).reshape((-1,) + (1,) * (len(shape) - 1 - dim))
    return level


def centred(stream_key, dims, scale, limit, cuts=(), kind=jnp.bfloat16):
    result = jax.random.normal(stream_key, dims, jnp.float32) * scale
    if len(cuts) > 0:
        result = steps_of(stream_key, dims, cuts, -0.22, 0.18) * result
    return jnp.clip(result, min=-limit, max=limit).astype(kind)


def setup_inputs(seed: int = 0) -> dict:
    seeds = jax.random.split(jax.random.key(seed), 9)
    return {
        "iterate": centred(seeds[0], (TOTAL_SLOTS, WINDOW_SLICES, 3, BLOCK_CELLS), 1.0, 6.0, ((0, 8), (1, 4)), jnp.float32),
        "forcing": centred(seeds[1], (TOTAL_SLOTS, WINDOW_SLICES, 3, BLOCK_CELLS), 1.0, 6.0, ((0, 8), (1, 4)), jnp.float32),
        "initial_velocity": centred(seeds[2], (TOTAL_SLOTS, 3, BLOCK_CELLS), 1.0, 6.0, ((0, 8),), jnp.float32),
        "viscosity": jnp.clip(jnp.exp(math.log(1.0) - 2.3025851 * jax.random.uniform(seeds[3], (TOTAL_SLOTS, BLOCK_CELLS), jnp.float32) ** steps_of(seeds[3], (TOTAL_SLOTS, BLOCK_CELLS), ((0, 8),), -0.2, 0.2)), 0.1, 1.0),
        "peclet": jnp.clip(jax.random.uniform(seeds[4], (TOTAL_SLOTS, 3, BLOCK_CELLS), jnp.float32, -0.9, 0.9) * steps_of(seeds[4], (TOTAL_SLOTS, 3, BLOCK_CELLS), ((0, 8),), -0.4, 0.0), -0.9, 0.9),
        "live_patch_mask": draw_live_patch_mask(jax.random.fold_in(seeds[8], 71), 0),
        "neighbour_holder": draw_neighbour_holder(jax.random.fold_in(seeds[8], 71), 0),
        "neighbour_slot": draw_neighbour_slot(jax.random.fold_in(seeds[8], 71), 0),
    }


STEP_DURATION = 0.5
ALPHA_SCALE = 0.1
HIGHEST_PRECISION = lax.Precision.HIGHEST


def face_layers(block_shaped):
    return jnp.stack([block_shaped[:, :, 0], block_shaped[:, :, -1], block_shaped[:, :, :, 0], block_shaped[:, :, :, -1], block_shaped[:, :, :, :, 0], block_shaped[:, :, :, :, -1]], axis=1)


def across_faces(block_shaped, neighbour_holder, neighbour_slot):
    patch_count = block_shaped.shape[0]
    channels = block_shaped.shape[1]
    layers = face_layers(block_shaped).reshape(patch_count * 6, channels, BLOCK_EDGE, BLOCK_EDGE)
    opposite = jnp.array([1, 0, 3, 2, 5, 4], dtype=jnp.int32)
    source = (jnp.maximum(neighbour_holder, 0) * SLOTS_PER_SPACE + jnp.maximum(neighbour_slot, 0)) * 6 + opposite[None, :]
    gathered = jnp.take(layers, source.reshape(-1).astype(jnp.int32), axis=0).reshape(patch_count, 6, channels, BLOCK_EDGE, BLOCK_EDGE)
    present = (neighbour_holder >= 0) & (neighbour_slot >= 0)
    return jnp.where(present[:, :, None, None, None], gathered, jnp.zeros_like(gathered))


def adjacent_total(block_shaped, ghost_faces, peclet_shaped):
    padded = jnp.pad(block_shaped, ((0, 0), (0, 0), (1, 1), (1, 1), (1, 1)))
    padded = padded.at[:, :, 0, 1:-1, 1:-1].set(ghost_faces[:, 0])
    padded = padded.at[:, :, -1, 1:-1, 1:-1].set(ghost_faces[:, 1])
    padded = padded.at[:, :, 1:-1, 0, 1:-1].set(ghost_faces[:, 2])
    padded = padded.at[:, :, 1:-1, -1, 1:-1].set(ghost_faces[:, 3])
    padded = padded.at[:, :, 1:-1, 1:-1, 0].set(ghost_faces[:, 4])
    padded = padded.at[:, :, 1:-1, 1:-1, -1].set(ghost_faces[:, 5])
    x_peclet = peclet_shaped[:, 0:1]
    y_peclet = peclet_shaped[:, 1:2]
    z_peclet = peclet_shaped[:, 2:3]
    summed = (1.0 - x_peclet) * padded[:, :, 2:, 1:-1, 1:-1] + (1.0 + x_peclet) * padded[:, :, :-2, 1:-1, 1:-1]
    summed = summed + (1.0 - y_peclet) * padded[:, :, 1:-1, 2:, 1:-1] + (1.0 + y_peclet) * padded[:, :, 1:-1, :-2, 1:-1]
    summed = summed + (1.0 - z_peclet) * padded[:, :, 1:-1, 1:-1, 2:] + (1.0 + z_peclet) * padded[:, :, 1:-1, 1:-1, :-2]
    return summed


def residual_grid(velocity_state, forcing_history, initial_velocity, viscosity, peclet_shaped, live_indicator, neighbour_holder, neighbour_slot):
    earlier = jnp.concatenate([initial_velocity[None], velocity_state[:-1]], axis=0)

    def one_slice(pieces):
        present_iterate, prior_velocity, right_hand_side = pieces
        block_shaped = present_iterate.reshape(TOTAL_SLOTS, 3, BLOCK_EDGE, BLOCK_EDGE, BLOCK_EDGE)
        ghost_faces = across_faces(block_shaped, neighbour_holder, neighbour_slot)
        adjacent_sum = adjacent_total(block_shaped, ghost_faces, peclet_shaped).reshape(TOTAL_SLOTS, 3, BLOCK_EDGE ** 3)
        operator_result = viscosity[:, None, :] * (6.0 * present_iterate - adjacent_sum)
        return (right_hand_side - (present_iterate - prior_velocity) / STEP_DURATION - operator_result) * live_indicator[:, None, None]

    return lax.map(one_slice, (velocity_state, earlier, forcing_history))


def solve_frequency(pieces, viscosity, peclet_shaped, neighbour_holder, neighbour_slot):
    source_real, source_imag, shift_real, shift_imag = pieces
    diagonal = shift_real + 6.0 * viscosity[:, None, :]
    determinant = diagonal * diagonal + shift_imag * shift_imag
    real_component = jnp.zeros_like(source_real)
    imaginary_component = jnp.zeros_like(source_imag)
    for sweep_index in range(SWEEPS):
        stacked_slices = jnp.stack([real_component, imaginary_component], axis=1).reshape(TOTAL_SLOTS, 6, BLOCK_EDGE, BLOCK_EDGE, BLOCK_EDGE)
        ghost_faces = across_faces(stacked_slices, neighbour_holder, neighbour_slot)
        adjacent_sum = adjacent_total(stacked_slices, ghost_faces, peclet_shaped).reshape(TOTAL_SLOTS, 2, 3, BLOCK_EDGE ** 3)
        total_real = source_real + viscosity[:, None, :] * adjacent_sum[:, 0]
        total_imag = source_imag + viscosity[:, None, :] * adjacent_sum[:, 1]
        real_component = (diagonal * total_real + shift_imag * total_imag) / determinant
        imaginary_component = (diagonal * total_imag - shift_imag * total_real) / determinant
    return real_component, imaginary_component


def reference(iterate, forcing, initial_velocity, viscosity, peclet, live_patch_mask, neighbour_holder, neighbour_slot):
    velocity_state = jnp.transpose(iterate, (1, 0, 2, 3))
    forcing_history = jnp.transpose(forcing, (1, 0, 2, 3))
    live_indicator = live_patch_mask.astype(jnp.float32)
    peclet_shaped = peclet.reshape(TOTAL_SLOTS, 3, BLOCK_EDGE, BLOCK_EDGE, BLOCK_EDGE)
    residual_value = residual_grid(velocity_state, forcing_history, initial_velocity, viscosity, peclet_shaped, live_indicator, neighbour_holder, neighbour_slot)
    times = jnp.arange(WINDOW_SLICES, dtype=jnp.int32)
    product = (times[:, None] * times[None, :]) % WINDOW_SLICES
    angles = 2.0 * jnp.pi * product.astype(jnp.float32) / WINDOW_SLICES
    ramp = times.astype(jnp.float32) / WINDOW_SLICES
    twisted = jnp.power(ALPHA_SCALE, ramp)
    untwisted = jnp.power(ALPHA_SCALE, -ramp) / WINDOW_SLICES
    cosine = jnp.cos(angles)
    sine = jnp.sin(angles)
    source_real = jnp.einsum("kl,lncx->kncx", cosine * twisted[None, :], residual_value, precision=HIGHEST_PRECISION)
    source_imag = jnp.einsum("kl,lncx->kncx", -sine * twisted[None, :], residual_value, precision=HIGHEST_PRECISION)
    root = ALPHA_SCALE ** (1.0 / WINDOW_SLICES)
    base_angle = 2.0 * jnp.pi * times.astype(jnp.float32) / WINDOW_SLICES
    shift_real = (1.0 - root * jnp.cos(base_angle)) / STEP_DURATION
    shift_imag = root * jnp.sin(base_angle) / STEP_DURATION
    solver = partial(solve_frequency, viscosity=viscosity, peclet_shaped=peclet_shaped, neighbour_holder=neighbour_holder, neighbour_slot=neighbour_slot)
    real_component, imaginary_component = lax.map(solver, (source_real, source_imag, shift_real, shift_imag))
    update = jnp.einsum("lk,kncx->lncx", cosine * untwisted[:, None], real_component, precision=HIGHEST_PRECISION)
    update = update + jnp.einsum("lk,kncx->lncx", -sine * untwisted[:, None], imaginary_component, precision=HIGHEST_PRECISION)
    advanced_state = velocity_state + update
    corrected_residual = residual_grid(advanced_state, forcing_history, initial_velocity, viscosity, peclet_shaped, live_indicator, neighbour_holder, neighbour_slot)
    return jnp.transpose(advanced_state, (1, 0, 2, 3)), jnp.transpose(corrected_residual, (1, 0, 2, 3))
```

```python
import jax
import jax.numpy as jnp
from jax import lax
from jax.experimental import pallas as pl
from jax.experimental.pallas import tpu as pltpu
from jax.sharding import PartitionSpec as P

EDGE = 16
LANES = 128
CHUNKS = 32
COMPONENTS = 3
ALPHA_SCALE = 0.1
WINDOW_SLICES = 16
SWEEPS = 5
XP, XM, YP, YM, ZP, ZM, XG, YG, ZG, Q, INV, K0 = range(12)
CORE, CHIP, SIDE_X, SIDE_Y, HOLD = range(5)
F32 = jnp.float32


def iota(shape, axis):
    return lax.broadcasted_iota(jnp.int32, shape, axis)


def tile_shape(*lead):
    return lead + (2, EDGE, LANES)


def call(kernel, flags, ins, outs, scratch=(), flops=2_000_000, name=None):
    vmem = pl.BlockSpec(memory_space=pltpu.VMEM)
    return pl.pallas_call(
        kernel,
        in_specs=[pl.BlockSpec(memory_space=pltpu.SMEM)] + [vmem] * len(ins),
        out_specs=[vmem] * len(outs),
        out_shape=[jax.ShapeDtypeStruct(s, F32) for s in outs],
        scratch_shapes=list(scratch),
        compiler_params=pltpu.CompilerParams(vmem_limit_bytes=24 * 1024 * 1024),
        cost_estimate=pl.CostEstimate(flops=flops, bytes_accessed=1_000_000, transcendentals=0),
        name=name,
    )(flags, *ins)


class Shape:
    def __init__(self, slots, local, n_time, places):
        self.slots = slots
        self.half = slots // 2
        self.local = local
        self.span = 2 * local
        self.chips = n_time // 2
        levels = places.bit_length() - 1
        self.bits = [[b for b in range(levels) if b % 3 == d] for d in range(3)]
        self.y_per = max(1, 8 // self.span)
        self.z_per = max(1, 16 // self.span)
        self.x_shape = (2 * COMPONENTS, self.span * 2, LANES)
        self.y_shape = (-(-2 // self.y_per) * COMPONENTS, EDGE, LANES)
        self.z_shape = tile_shape(-(-self.half // self.z_per) * COMPONENTS)
        self.x_count = len(self.bits[0])
        self.field = tile_shape(self.half, COMPONENTS, self.span)
        self.slice = tile_shape(self.half, COMPONENTS)


def position(place, bits):
    if len(bits) == 1:
        return place >> bits[0] & 1
    low, high = place >> bits[0] & 1, place >> bits[1] & 1
    return 2 * high + (low ^ high)


def exchange(sh, messages, n_time, places):
    axes = ("tm", "space")
    received = []
    x_out, y_out, inner_out, z_out = messages[:-3], messages[-3], messages[-2], messages[-1]

    def pairs(bit, bits, crossed):
        table = []
        for t in range(n_time):
            for s in range(places):
                here, there = position(s, bits), position(s ^ (1 << bit), bits)
                if abs(here - there) != 1:
                    continue
                if crossed and (there > here) != (t % 2 == 1):
                    continue
                target = t ^ 1 if crossed else t
                table.append((t * places + s, target * places + (s ^ (1 << bit))))
        return table

    z_in = lax.ppermute(z_out, axes, pairs(sh.bits[2][0], sh.bits[2], True))
    x_in = [
        lax.ppermute(x_out[i], axes, pairs(bit, sh.bits[0], False))
        for i, bit in enumerate(sh.bits[0])
    ]
    y_in = lax.ppermute(y_out, axes, pairs(sh.bits[1][0], sh.bits[1], False))
    inner_in = swap_cores(inner_out, n_time)
    return x_in + [y_in, inner_in, z_in]


def swap_cores(value, n_time):
    return lax.ppermute(value, "tm", [(t, t ^ 1) for t in range(n_time)])


def emit_messages(sh, flags, src, outs):
    core = flags[CORE]
    lane = iota((EDGE, LANES), 1)
    x_outs, y_out, inner_out, z_out = outs[:-3], outs[-3], outs[-2], outs[-1]
    side_y = flags[SIDE_Y]

    def comp_step(comp, _):
        for number, x_out in enumerate(x_outs):
            side = flags[SIDE_X] if number == 0 else 1 - flags[SIDE_X]
            for jj in range(2):
                for l in range(sh.span):
                    for h in range(2):
                        upper = src[2 * jj + 1, comp, l, h, EDGE - 1 : EDGE, :]
                        lower = src[2 * jj, comp, l, h, 0:1, :]
                        x_out[jj * COMPONENTS + comp, 2 * l + h : 2 * l + h + 1, :] = jnp.where(
                            side == 1, upper, lower
                        )
        group_of_lane = lane // EDGE
        for g in range(-(-2 // sh.y_per)):
            packed = jnp.zeros((EDGE, LANES), F32)
            for jj in range(g * sh.y_per, min(2, (g + 1) * sh.y_per)):
                for l in range(sh.span):
                    index = (jj % sh.y_per) * sh.span + l
                    layer = src[2 * side_y + jj, comp, l, side_y]
                    if index:
                        layer = pltpu.roll(layer, EDGE * index, 1)
                    packed = jnp.where(group_of_lane == (index + 7 * side_y) % 8, layer, packed)
            y_out[g * COMPONENTS + comp] = jnp.where(
                side_y == 1, pltpu.roll(packed, EDGE, 1), packed
            )
        within = lane % EDGE
        for g in range(-(-sh.half // sh.z_per)):
            for h in range(2):
                low = jnp.zeros((EDGE, LANES), F32)
                high = jnp.zeros((EDGE, LANES), F32)
                for j in range(g * sh.z_per, min(sh.half, (g + 1) * sh.z_per)):
                    for l in range(sh.span):
                        index = (j % sh.z_per) * sh.span + l
                        tile = src[j, comp, l, h]
                        here = within == index
                        shifted = pltpu.roll(tile, index, 1) if index else tile
                        low = jnp.where(here, shifted, low)
                        back = (index - EDGE + 1) % LANES
                        shifted = pltpu.roll(tile, back, 1) if back else tile
                        high = jnp.where(here, shifted, high)
                inner_out[g * COMPONENTS + comp, h] = jnp.where(core == 1, low, high)
                z_out[g * COMPONENTS + comp, h] = jnp.where(core == 1, high, low)
        return 0

    lax.fori_loop(0, COMPONENTS, comp_step, 0)


def neighbour_sum(sh, flags, coef, src, faces, z_ghost, j, comp, l):
    xs, y_in = faces[:-1], faces[-1]
    lane = iota((EDGE, LANES), 1)
    tiles = [src[j, comp, l, h] for h in range(2)]
    up = [pltpu.roll(v, LANES - EDGE, 1) for v in tiles]
    down = [pltpu.roll(v, EDGE, 1) for v in tiles]
    y_upper = [jnp.where(lane < LANES - EDGE, up[0], up[1]), up[1]]
    y_lower = [down[0], jnp.where(lane >= EDGE, down[1], down[0])]
    x_side, x_row = j % 2, j // 2
    y_side, y_row = j // 2, j % 2
    y_index = (y_row % sh.y_per) * sh.span + l
    y_group = y_in[(y_row // sh.y_per) * COMPONENTS + comp]
    if y_side == 1:
        y_ghost = [
            pltpu.roll(src[j ^ 2, comp, l, 1], EDGE, 1),
            pltpu.roll(y_group, (LANES - EDGE - EDGE * y_index) % LANES, 1)
            if (LANES - EDGE - EDGE * y_index) % LANES
            else y_group,
        ]
    else:
        y_ghost = [
            pltpu.roll(y_group, (-EDGE * y_index) % LANES, 1) if y_index else y_group,
            pltpu.roll(src[j ^ 2, comp, l, 0], LANES - EDGE, 1),
        ]
    z_index = (j % sh.z_per) * sh.span + l
    z_group = (j // sh.z_per) * COMPONENTS + comp
    result = []
    for h in range(2):
        v = tiles[h]
        total = coef[j, XP, h] * pltpu.roll(v, EDGE - 1, 0)
        total += coef[j, XM, h] * pltpu.roll(v, 1, 0)
        total += coef[j, YP, h] * y_upper[h]
        total += coef[j, YM, h] * y_lower[h]
        total += coef[j, ZP, h] * pltpu.roll(v, LANES - 1, 1)
        total += coef[j, ZM, h] * pltpu.roll(v, 1, 1)
        total += coef[j, YG, h] * y_ghost[h]
        low = z_ghost[0, z_group, h]
        low = pltpu.roll(low, LANES - z_index, 1) if z_index else low
        high = z_ghost[1, z_group, h]
        high = pltpu.roll(high, EDGE - 1 - z_index, 1) if z_index != EDGE - 1 else high
        total += coef[j, ZG, h] * jnp.where(lane % EDGE == 0, low, high)
        outer = x_row * COMPONENTS + comp
        row = slice(2 * l + h, 2 * l + h + 1)
        if len(xs) == 1:
            crossed = xs[0][outer, row, :]
        else:
            wanted = flags[SIDE_X] if x_side == 1 else 1 - flags[SIDE_X]
            crossed = jnp.where(wanted == 1, xs[0][outer, row, :], xs[1][outer, row, :])
        inside = EDGE - 1 if x_side == 1 else 0
        own = src[j ^ 1, comp, l, h, inside : inside + 1, :]
        first, last = (own, crossed) if x_side == 1 else (crossed, own)
        ghost = jnp.concatenate(
            [jnp.broadcast_to(first, (8, LANES)), jnp.broadcast_to(last, (8, LANES))], axis=0
        )
        total += coef[j, XG, h] * ghost
        result.append(total)
    return result


def place_z_ghost(flags, inner_in, z_in, z_ghost):
    core = flags[CORE]

    def step(g, _):
        inner, outer = inner_in[g], z_in[g]
        z_ghost[0, g] = jnp.where(core == 1, inner, outer)
        z_ghost[1, g] = jnp.where(core == 1, outer, inner)
        return 0

    lax.fori_loop(0, inner_in.shape[0], step, 0)


def rows_to_tiles(read, count, rows, write):
    for chunk in range(CHUNKS):
        rows[chunk * count : (chunk + 1) * count, :] = read(chunk)
    for i in range(count):
        for h in range(2):
            write(i, h, rows[pl.ds(h * count + i, EDGE, 2 * count), :])


def tiles_to_rows(tile, count, rows, write):
    for i in range(count):
        for h in range(2):
            rows[pl.ds(h * count + i, EDGE, 2 * count), :] = tile(i, h)
    for chunk in range(CHUNKS):
        write(chunk, rows[chunk * count : (chunk + 1) * count, :])


def coefficient_kernel(sh, flags, viscosity, peclet, initial, coef, first, rows, tiles):
    core = flags[CORE]
    chip = flags[CHIP]
    slots = sh.slots

    def unpack(source, kind):
        def write(i, h, value):
            tiles[kind, i, h] = value

        rows_to_tiles(lambda c: source(c), slots, rows, write)

    unpack(lambda c: viscosity[:, c * LANES : (c + 1) * LANES], 0)
    for d in range(3):
        unpack(lambda c, d=d: peclet[d, :, c * LANES : (c + 1) * LANES], 1 + d)
    for d in range(3):
        unpack(lambda c, d=d: initial[d, :, c * LANES : (c + 1) * LANES], 4 + d)

    lane = iota((EDGE, LANES), 1)
    row = iota((EDGE, LANES), 0)
    zero = jnp.zeros((EDGE, LANES), F32)

    def step(j, _):
        slot = core * sh.half + j
        hold = [flags[HOLD + j * 6 + face].astype(F32) for face in range(6)]
        for h in range(2):
            nu = tiles[0, slot, h]
            inverse = 2.0 + 6.0 * nu
            q = 2.0 / inverse
            scale = nu / inverse
            plus = [scale * (1.0 - tiles[1 + d, slot, h]) for d in range(3)]
            minus = [scale * (1.0 + tiles[1 + d, slot, h]) for d in range(3)]
            coef[j, XP, h] = jnp.where(row < EDGE - 1, plus[0], zero)
            coef[j, XM, h] = jnp.where(row > 0, minus[0], zero)
            coef[j, XG, h] = jnp.where(
                row == 0,
                minus[0] * hold[0],
                jnp.where(row == EDGE - 1, plus[0] * hold[1], zero),
            )
            if h == 0:
                coef[j, YP, h] = plus[1]
                coef[j, YM, h] = jnp.where(lane >= EDGE, minus[1], zero)
                coef[j, YG, h] = jnp.where(lane < EDGE, minus[1] * hold[2], zero)
            else:
                coef[j, YP, h] = jnp.where(lane < LANES - EDGE, plus[1], zero)
                coef[j, YM, h] = minus[1]
                coef[j, YG, h] = jnp.where(lane >= LANES - EDGE, plus[1] * hold[3], zero)
            within = lane % EDGE
            coef[j, ZP, h] = jnp.where(within < EDGE - 1, plus[2], zero)
            coef[j, ZM, h] = jnp.where(within > 0, minus[2], zero)
            coef[j, ZG, h] = jnp.where(
                within == 0,
                minus[2] * hold[4],
                jnp.where(within == EDGE - 1, plus[2] * hold[5], zero),
            )
            coef[j, Q, h] = q
            coef[j, INV, h] = inverse
            power = q
            for _ in range(sh.span.bit_length() - 1):
                power = power * power
            whole = power
            for _ in range(sh.chips.bit_length() - 1):
                whole = whole * whole
            weight = 1.0 / (1.0 - ALPHA_SCALE * whole)
            for back in range(1, sh.chips + 1):
                wrapped = jnp.where(chip < back, ALPHA_SCALE, 1.0)
                coef[j, K0 + back - 1, h] = weight * wrapped
                weight = weight * power
            for d in range(COMPONENTS):
                first[j, d, h] = tiles[4 + d, slot, h]
        return 0

    lax.fori_loop(0, sh.half, step, 0)


def gather_kernel(sh, flags, whole, other, field, last, *rest):
    rows = rest[-1]
    core = flags[CORE]

    def step(k, _):
        j, comp = k // COMPONENTS, k % COMPONENTS

        def own(i, h, value):
            field[j, comp, core * sh.local + i, h] = value

        def partner(i, h, value):
            field[j, comp, (1 - core) * sh.local + i, h] = value

        slot = core * sh.half + j
        rows_to_tiles(
            lambda c: whole[slot, comp, :, c * LANES : (c + 1) * LANES], sh.local, rows.at[0], own
        )
        rows_to_tiles(
            lambda c: other[j, comp, :, c * LANES : (c + 1) * LANES], sh.local, rows.at[1], partner
        )
        last[j, comp] = field[j, comp, sh.span - 1]
        return 0

    lax.fori_loop(0, sh.half * COMPONENTS, step, 0)
    emit_messages(sh, flags, field, rest[:-1])


def force_kernel(sh, flags, whole, other, field, rows):
    core = flags[CORE]

    def step(k, _):
        j, comp = k // COMPONENTS, k % COMPONENTS

        def own(i, h, value):
            field[j, comp, core * sh.local + i, h] = value

        def partner(i, h, value):
            field[j, comp, (1 - core) * sh.local + i, h] = value

        slot = core * sh.half + j
        rows_to_tiles(
            lambda c: whole[slot, comp, :, c * LANES : (c + 1) * LANES], sh.local, rows.at[0], own
        )
        rows_to_tiles(
            lambda c: other[j, comp, :, c * LANES : (c + 1) * LANES], sh.local, rows.at[1], partner
        )
        return 0

    lax.fori_loop(0, sh.half * COMPONENTS, step, 0)


def residual_kernel(sh, flags, coef, field, force, before, first, *rest):
    faces = rest[: sh.x_count + 1]
    inner_in, z_in, scaled, partial, last, z_ghost = rest[sh.x_count + 1 :]
    place_z_ghost(flags, inner_in, z_in, z_ghost)
    chip = flags[CHIP]
    for j in range(sh.half):
        live = flags[HOLD + 6 * sh.half + j].astype(F32)

        def comp_step(comp, _, j=j, live=live):
            prior = [jnp.where(chip == 0, first[j, comp, h], before[j, comp, h]) for h in range(2)]
            carry = [jnp.zeros((EDGE, LANES), F32)] * 2
            for l in range(sh.span):
                total = neighbour_sum(sh, flags, coef, field, faces, z_ghost, j, comp, l)
                for h in range(2):
                    q = coef[j, Q, h]
                    now = field[j, comp, l, h]
                    value = total[h] + (0.5 * q) * force[j, comp, l, h] - now + q * prior[h]
                    value = value * live
                    prior[h] = now
                    scaled[j, comp, l, h] = value
                    carry[h] = value + q * carry[h]
                    partial[j, comp, l, h] = carry[h]
            for h in range(2):
                last[j, comp, h] = carry[h]
            return 0

        lax.fori_loop(0, COMPONENTS, comp_step, 0)


def sweep_kernel(sh, flags, coef, field, scaled, *rest):
    faces = rest[: sh.x_count + 1]
    inner_in, z_in, partial, last, z_ghost = rest[sh.x_count + 1 :]
    place_z_ghost(flags, inner_in, z_in, z_ghost)
    for j in range(sh.half):

        def comp_step(comp, _, j=j):
            carry = [jnp.zeros((EDGE, LANES), F32)] * 2
            for l in range(sh.span):
                total = neighbour_sum(sh, flags, coef, field, faces, z_ghost, j, comp, l)
                for h in range(2):
                    carry[h] = scaled[j, comp, l, h] + total[h] + coef[j, Q, h] * carry[h]
                    partial[j, comp, l, h] = carry[h]
            for h in range(2):
                last[j, comp, h] = carry[h]
            return 0

        lax.fori_loop(0, COMPONENTS, comp_step, 0)


def incoming_slice(sh, coef, lasts, j, comp, h):
    total = coef[j, K0, h] * lasts[0][j, comp, h]
    for back in range(1, sh.chips):
        total += coef[j, K0 + back, h] * lasts[back][j, comp, h]
    return total


def close_kernel(sh, flags, coef, partial, *rest):
    lasts, (field, *messages) = rest[: sh.chips], rest[sh.chips :]

    def step(k, _):
        j, comp = k // COMPONENTS, k % COMPONENTS
        for h in range(2):
            q = coef[j, Q, h]
            term = incoming_slice(sh, coef, lasts, j, comp, h)
            for l in range(sh.span):
                term = q * term
                field[j, comp, l, h] = partial[j, comp, l, h] + term
        return 0

    lax.fori_loop(0, sh.half * COMPONENTS, step, 0)
    emit_messages(sh, flags, field, messages)


def velocity_kernel(sh, flags, velocity, field, keep, send, rows):
    core = flags[CORE]

    def step(k, _):
        j, comp = k // COMPONENTS, k % COMPONENTS
        for which, out in ((core, keep), (1 - core, send)):

            def tile(i, h, which=which):
                l = which * sh.local + i
                return velocity[j, comp, l, h] + field[j, comp, l, h]

            def write(c, value, out=out):
                out[j, comp, :, c * LANES : (c + 1) * LANES] = value

            tiles_to_rows(tile, sh.local, rows.at[0 if out is keep else 1], write)
        return 0

    lax.fori_loop(0, sh.half * COMPONENTS, step, 0)


def final_kernel(sh, flags, coef, field, scaled, *rest):
    lasts, rest = rest[: sh.chips], rest[sh.chips :]
    faces = rest[: sh.x_count + 1]
    inner_in, z_in, keep, send, z_ghost, hold, rows = rest[sh.x_count + 1 :]
    place_z_ghost(flags, inner_in, z_in, z_ghost)
    core = flags[CORE]
    chip = flags[CHIP]
    for j in range(sh.half):
        live = flags[HOLD + 6 * sh.half + j].astype(F32)

        def comp_step(comp, _, j=j, live=live):
            prior = [
                jnp.where(chip == 0, 0.0, incoming_slice(sh, coef, lasts, j, comp, h))
                for h in range(2)
            ]
            for l in range(sh.span):
                total = neighbour_sum(sh, flags, coef, field, faces, z_ghost, j, comp, l)
                for h in range(2):
                    now = field[j, comp, l, h]
                    value = scaled[j, comp, l, h] + total[h] - now + coef[j, Q, h] * prior[h]
                    prior[h] = now
                    hold[l, h] = value * (coef[j, INV, h] * live)
            for which, out in ((core, keep), (1 - core, send)):

                def tile(i, h, which=which):
                    return hold[which * sh.local + i, h]

                def write(c, value, out=out):
                    out[j, comp, :, c * LANES : (c + 1) * LANES] = value

                tiles_to_rows(tile, sh.local, rows.at[0 if out is keep else 1], write)
            return 0

        lax.fori_loop(0, COMPONENTS, comp_step, 0)


def bind(kernel, sh):
    def run(*refs):
        kernel(sh, *refs)

    return run


def body(
    iterate,
    forcing,
    initial_velocity,
    viscosity,
    peclet,
    live_patch_mask,
    neighbour_holder,
    neighbour_slot,
):
    n_time, places = lax.axis_size("tm"), lax.axis_size("space")
    slots, local = iterate.shape[:2]
    sh = Shape(slots, local, n_time, places)
    half = sh.half
    t, place = lax.axis_index("tm"), lax.axis_index("space")
    core, chip = t % 2, t // 2
    velocity = iterate.transpose(0, 2, 1, 3)
    force = forcing.transpose(0, 2, 1, 3)

    def partner_slots(value):
        return swap_cores(lax.dynamic_slice_in_dim(value, (1 - core) * half, half, 0), n_time)

    velocity_other = partner_slots(velocity)
    force_other = partner_slots(force)

    def side(bits):
        return 1 - position(place, bits) % 2

    held = lax.dynamic_slice_in_dim(neighbour_holder, core * half, half, 0) >= 0
    live = lax.dynamic_slice_in_dim(live_patch_mask, core * half, half, 0)
    flags = jnp.concatenate(
        [
            jnp.stack([core, chip, side(sh.bits[0]), side(sh.bits[1])]).astype(jnp.int32),
            held.astype(jnp.int32).reshape(-1),
            live.astype(jnp.int32),
        ]
    )
    rows = pltpu.VMEM((2, CHUNKS * local, LANES), F32)
    z_ghost = pltpu.VMEM((2,) + sh.z_shape, F32)
    messages = [sh.x_shape] * sh.x_count + [sh.y_shape, sh.z_shape, sh.z_shape]

    coef, first = call(
        bind(coefficient_kernel, sh),
        flags,
        [viscosity, peclet.transpose(1, 0, 2), initial_velocity.transpose(1, 0, 2)],
        [tile_shape(half, K0 + sh.chips), sh.slice],
        [pltpu.VMEM((CHUNKS * slots, LANES), F32), pltpu.VMEM(tile_shape(7, slots), F32)],
        name="coefficients",
    )
    field, last, *out = call(
        bind(gather_kernel, sh),
        flags,
        [velocity, velocity_other],
        [sh.field, sh.slice] + messages,
        [rows],
        name="gather",
    )
    before = lax.ppermute(last, "tm", [(a, a + 2) for a in range(n_time - 2)])
    faces = exchange(sh, out, n_time, places)
    (pushed,) = call(
        bind(force_kernel, sh), flags, [force, force_other], [sh.field], [rows], name="force"
    )
    scaled, partial, last = call(
        bind(residual_kernel, sh),
        flags,
        [coef, field, pushed, before, first] + faces,
        [sh.field, sh.field, sh.slice],
        [z_ghost],
        flops=8_000_000,
        name="residual",
    )

    def chip_ends(last):
        return [
            lax.ppermute(last, "tm", [(a, (a + 2 * back) % n_time) for a in range(n_time)])
            for back in range(1, sh.chips)
        ] + [last]

    correction = None
    for sweep in range(SWEEPS):
        if sweep > 0:
            partial, last = call(
                bind(sweep_kernel, sh),
                flags,
                [coef, correction, scaled] + faces,
                [sh.field, sh.slice],
                [z_ghost],
                flops=8_000_000,
                name="sweep",
            )
        ends = chip_ends(last)
        correction, *out = call(
            bind(close_kernel, sh),
            flags,
            [coef, partial] + ends,
            [sh.field] + messages,
            name="close",
        )
        faces = exchange(sh, out, n_time, places)
    native = (half, COMPONENTS, local, CHUNKS * LANES)
    keep, send = call(
        bind(velocity_kernel, sh),
        flags,
        [field, correction],
        [native, native],
        [rows],
        name="velocity",
    )

    def restore(keep, send):
        other = swap_cores(send, n_time)
        first_core = core == 0
        whole = jnp.concatenate(
            [jnp.where(first_core, keep, other), jnp.where(first_core, other, keep)], axis=0
        )
        return whole.transpose(0, 2, 1, 3)

    corrected_velocity = restore(keep, send)
    keep, send = call(
        bind(final_kernel, sh),
        flags,
        [coef, correction, scaled] + ends + faces,
        [native, native],
        [z_ghost, pltpu.VMEM(tile_shape(sh.span), F32), rows],
        flops=8_000_000,
        name="final",
    )
    return corrected_velocity, restore(keep, send)


def solution(mesh):
    return jax.shard_map(
        body,
        mesh=mesh,
        in_specs=(
            P("space", "tm", None, None),
            P("space", "tm", None, None),
            P("space", None, None),
            P("space", None),
            P("space", None, None),
            P("space"),
            P("space", None),
            P("space", None),
        ),
        out_specs=(P("space", "tm", None, None), P("space", "tm", None, None)),
        check_vma=False,
    )
```

```python
import jax
import jax.numpy as jnp
from jax import lax
from jax.experimental import pallas as pl
from jax.experimental.pallas import tpu as pltpu
from jax.sharding import PartitionSpec as P

EDGE = 16
LANES = 128
CHUNKS = 32
COMPONENTS = 3
ALPHA_SCALE = 0.1
WINDOW_SLICES = 16
SWEEPS = 5
XP, XM, YP, YM, ZP, ZM, XG, YG, ZG, Q, INV, K0 = range(12)
CORE, CHIP, SIDE_X, SIDE_Y, HOLD = range(5)
F32 = jnp.float32


def iota(shape, axis):
    return lax.broadcasted_iota(jnp.int32, shape, axis)


def tile_shape(*lead):
    return lead + (2, EDGE, LANES)


def call(kernel, flags, ins, outs, scratch=(), flops=2_000_000, name=None):
    vmem = pl.BlockSpec(memory_space=pltpu.VMEM)
    return pl.pallas_call(
        kernel,
        in_specs=[pl.BlockSpec(memory_space=pltpu.SMEM)] + [vmem] * len(ins),
        out_specs=[vmem] * len(outs),
        out_shape=[jax.ShapeDtypeStruct(s, F32) for s in outs],
        scratch_shapes=list(scratch),
        compiler_params=pltpu.CompilerParams(vmem_limit_bytes=24 * 1024 * 1024),
        cost_estimate=pl.CostEstimate(flops=flops, bytes_accessed=1_000_000, transcendentals=0),
        name=name,
    )(flags, *ins)


class Shape:
    def __init__(self, slots, local, n_time, places):
        self.slots = slots
        self.half = slots // 2
        self.local = local
        self.span = 2 * local
        self.chips = n_time // 2
        levels = places.bit_length() - 1
        self.bits = [[b for b in range(levels) if b % 3 == d] for d in range(3)]
        self.y_per = max(1, 8 // self.span)
        self.z_per = max(1, 16 // self.span)
        self.x_shape = (2 * COMPONENTS, self.span * 2, LANES)
        self.y_shape = (-(-2 // self.y_per) * COMPONENTS, EDGE, LANES)
        self.z_shape = tile_shape(-(-self.half // self.z_per) * COMPONENTS)
        self.x_count = len(self.bits[0])
        self.field = tile_shape(self.half, COMPONENTS, self.span)
        self.slice = tile_shape(self.half, COMPONENTS)


def position(place, bits):
    if len(bits) == 1:
        return place >> bits[0] & 1
    low, high = place >> bits[0] & 1, place >> bits[1] & 1
    return 2 * high + (low ^ high)


def exchange(sh, messages, n_time, places):
    axes = ("tm", "space")
    received = []
    x_out, y_out, inner_out, z_out = messages[:-3], messages[-3], messages[-2], messages[-1]

    def pairs(bit, bits, crossed):
        table = []
        for t in range(n_time):
            for s in range(places):
                here, there = position(s, bits), position(s ^ (1 << bit), bits)
                if abs(here - there) != 1:
                    continue
                if crossed and (there > here) != (t % 2 == 1):
                    continue
                target = t ^ 1 if crossed else t
                table.append((t * places + s, target * places + (s ^ (1 << bit))))
        return table

    z_in = lax.ppermute(z_out, axes, pairs(sh.bits[2][0], sh.bits[2], True))
    x_in = [
        lax.ppermute(x_out[i], axes, pairs(bit, sh.bits[0], False))
        for i, bit in enumerate(sh.bits[0])
    ]
    y_in = lax.ppermute(y_out, axes, pairs(sh.bits[1][0], sh.bits[1], False))
    inner_in = swap_cores(inner_out, n_time)
    return x_in + [y_in, inner_in, z_in]


def swap_cores(value, n_time):
    return lax.ppermute(value, "tm", [(t, t ^ 1) for t in range(n_time)])


def pack_faces(sh, flags, tile, src, outs):
    core = flags[CORE]
    lane = iota((EDGE, LANES), 1)
    within, group_of_lane = lane % EDGE, lane // EDGE
    x_outs, y_out, inner_out, z_out = outs[:-3], outs[-3], outs[-2], outs[-1]
    side_y = flags[SIDE_Y]
    y_groups = -(-2 // sh.y_per)

    for g in range(-(-sh.half // sh.z_per)):
        slots = range(g * sh.z_per, min(sh.half, (g + 1) * sh.z_per))

        def comp_step(comp, _, g=g, slots=slots):
            low = [jnp.zeros((EDGE, LANES), F32)] * 2
            high = [jnp.zeros((EDGE, LANES), F32)] * 2
            for j in slots:
                for l in range(sh.span):
                    index = (j % sh.z_per) * sh.span + l
                    for h in range(2):
                        value = tile(j, comp, l, h)
                        value = pltpu.roll(value, index, 1) if index else value
                        low[h] = jnp.where(within == index, value, low[h])
                        high[h] = jnp.where(within == (index + EDGE - 1) % EDGE, value, high[h])
            for h in range(2):
                inner_out[g * COMPONENTS + comp, h] = jnp.where(core == 1, low[h], high[h])
                z_out[g * COMPONENTS + comp, h] = jnp.where(core == 1, high[h], low[h])
            for number, x_out in enumerate(x_outs):
                side = flags[SIDE_X] if number == 0 else 1 - flags[SIDE_X]
                for jj in range(slots[0] // 2, slots[-1] // 2 + 1):
                    for l in range(sh.span):
                        for h in range(2):
                            upper = src[2 * jj + 1, comp, l, h, EDGE - 1 : EDGE, :]
                            lower = src[2 * jj, comp, l, h, 0:1, :]
                            row = slice(2 * l + h, 2 * l + h + 1)
                            x_out[jj * COMPONENTS + comp, row, :] = jnp.where(
                                side == 1, upper, lower
                            )
            for half in range(slots[0] // 2, slots[-1] // 2 + 1):

                @pl.when(side_y == half)
                def _(half=half):
                    for y in range(y_groups):
                        packed = jnp.zeros((EDGE, LANES), F32)
                        for jj in range(y * sh.y_per, min(2, (y + 1) * sh.y_per)):
                            for l in range(sh.span):
                                index = (jj % sh.y_per) * sh.span + l
                                layer = src[2 * half + jj, comp, l, half]
                                shift = EDGE * (index + half) % LANES
                                layer = pltpu.roll(layer, shift, 1) if shift else layer
                                packed = jnp.where(group_of_lane == index, layer, packed)
                        y_out[y * COMPONENTS + comp] = packed

            return 0

        lax.fori_loop(0, COMPONENTS, comp_step, 0)


def inner_sum(sh, flags, coef, src, j, comp, l):
    lane = iota((EDGE, LANES), 1)
    row = iota((EDGE, LANES), 0)
    within = lane % EDGE
    hold = [flags[HOLD + j * 6 + face].astype(F32) for face in range(4)]
    tiles = [src[j, comp, l, h] for h in range(2)]
    if j // 2 == 0:
        below, above = 0.0, src[j ^ 2, comp, l, 0] * hold[3]
    else:
        below, above = src[j ^ 2, comp, l, 1] * hold[2], 0.0
    y_next = [jnp.where(lane < EDGE, tiles[1], tiles[0]), jnp.where(lane < EDGE, above, tiles[1])]
    last = lane >= LANES - EDGE
    y_back = [jnp.where(last, below, tiles[0]), jnp.where(last, tiles[0], tiles[1])]
    result = []
    for h in range(2):
        v = tiles[h]
        if j % 2 == 0:
            before, after = 0.0, src[j ^ 1, comp, l, h, 0:1, :] * hold[1]
        else:
            before, after = src[j ^ 1, comp, l, h, EDGE - 1 : EDGE, :] * hold[0], 0.0
        total = coef[j, YP, h] * pltpu.roll(y_next[h], LANES - EDGE, 1)
        total += coef[j, YM, h] * pltpu.roll(y_back[h], EDGE, 1)
        total += coef[j, ZP, h] * pltpu.roll(v, LANES - 1, 1)
        total += coef[j, ZM, h] * pltpu.roll(v, 1, 1)
        total += coef[j, XP, h] * pltpu.roll(jnp.where(row == 0, after, v), EDGE - 1, 0)
        total += coef[j, XM, h] * pltpu.roll(jnp.where(row == EDGE - 1, before, v), 1, 0)
        result.append(total)
    return result


def ghost_sum(sh, flags, coef, faces, z_ghost, total, j, comp, l):
    xs, y_in = faces[:-1], faces[-1]
    x_side, x_row = j % 2, j // 2
    y_side, y_row = j // 2, j % 2
    y_index = (y_row % sh.y_per) * sh.span + l
    z_index = (j % sh.z_per) * sh.span + l
    z_group = (j // sh.z_per) * COMPONENTS + comp
    outer = x_row * COMPONENTS + comp
    result = []
    for h in range(2):
        value = total[h]
        value += coef[j, ZG, h] * pltpu.roll(
            z_ghost[z_index % 2, z_group, h], LANES - EDGE + 1 - z_index, 1
        )
        if h == y_side:
            group = y_in[(y_row // sh.y_per) * COMPONENTS + comp]
            shift = ((LANES - EDGE if y_side else 0) - EDGE * y_index) % LANES
            value += coef[j, YG, h] * (pltpu.roll(group, shift, 1) if shift else group)
        row = slice(2 * l + h, 2 * l + h + 1)
        if len(xs) == 1:
            crossed = xs[0][outer, row, :]
        else:
            wanted = flags[SIDE_X] if x_side == 1 else 1 - flags[SIDE_X]
            crossed = jnp.where(wanted == 1, xs[0][outer, row, :], xs[1][outer, row, :])
        part = slice(8 * x_side, 8 * x_side + 8)
        changed = value[part] + coef[j, XG, h, part, :] * jnp.broadcast_to(crossed, (8, LANES))
        parts = [value[:8], changed] if x_side else [changed, value[8:]]
        result.append(jnp.concatenate(parts, axis=0))
    return result


def place_z_ghost(flags, inner_in, z_in, z_ghost):
    core = flags[CORE]
    odd = iota((EDGE, LANES), 1) % 2 == 1

    def step(g, _):
        for h in range(2):
            inner, outer = inner_in[g, h], z_in[g, h]
            upper = pltpu.roll(jnp.where(core == 1, outer, inner), 2 * EDGE - 2, 1)
            lower = jnp.where(core == 1, inner, outer)
            z_ghost[0, g, h] = jnp.where(odd, lower, upper)
            z_ghost[1, g, h] = jnp.where(odd, upper, lower)
        return 0

    lax.fori_loop(0, inner_in.shape[0], step, 0)


def rows_to_tiles(read, count, rows, write):
    for chunk in range(CHUNKS):
        rows[chunk * count : (chunk + 1) * count, :] = read(chunk)
    for i in range(count):
        for h in range(2):
            write(i, h, rows[pl.ds(h * count + i, EDGE, 2 * count), :])


def tiles_to_rows(tile, count, rows, write):
    for i in range(count):
        for h in range(2):
            rows[pl.ds(h * count + i, EDGE, 2 * count), :] = tile(i, h)
    for chunk in range(CHUNKS):
        write(chunk, rows[chunk * count : (chunk + 1) * count, :])


def coefficient_kernel(sh, flags, viscosity, peclet, initial, coef, first, rows, tiles):
    core = flags[CORE]
    chip = flags[CHIP]
    slots = sh.slots

    def unpack(source, kind):
        def write(i, h, value):
            tiles[kind, i, h] = value

        rows_to_tiles(lambda c: source(c), slots, rows, write)

    unpack(lambda c: viscosity[:, c * LANES : (c + 1) * LANES], 0)
    for d in range(3):
        unpack(lambda c, d=d: peclet[d, :, c * LANES : (c + 1) * LANES], 1 + d)
    for d in range(3):
        unpack(lambda c, d=d: initial[d, :, c * LANES : (c + 1) * LANES], 4 + d)

    lane = iota((EDGE, LANES), 1)
    row = iota((EDGE, LANES), 0)
    within = lane % EDGE
    zero = jnp.zeros((EDGE, LANES), F32)

    def step(j, _):
        slot = core * sh.half + j
        hold = [flags[HOLD + j * 6 + face].astype(F32) for face in range(6)]
        for h in range(2):
            nu = tiles[0, slot, h]
            inverse = 2.0 + 6.0 * nu
            q = 2.0 / inverse
            scale = nu / inverse
            plus = [scale * (1.0 - tiles[1 + d, slot, h]) for d in range(3)]
            minus = [scale * (1.0 + tiles[1 + d, slot, h]) for d in range(3)]
            for d, (upper, lower) in enumerate(((XP, XM), (YP, YM), (ZP, ZM))):
                coef[j, upper, h] = plus[d]
                coef[j, lower, h] = minus[d]
            coef[j, ZP, h] = jnp.where(within < EDGE - 1, plus[2], zero)
            coef[j, ZM, h] = jnp.where(within > 0, minus[2], zero)
            coef[j, XG, h] = jnp.where(
                row == 0,
                minus[0] * hold[0],
                jnp.where(row == EDGE - 1, plus[0] * hold[1], zero),
            )
            if h == 0:
                coef[j, YG, h] = jnp.where(lane < EDGE, minus[1] * hold[2], zero)
            else:
                coef[j, YG, h] = jnp.where(lane >= LANES - EDGE, plus[1] * hold[3], zero)
            coef[j, ZG, h] = jnp.where(
                within == 0,
                minus[2] * hold[4],
                jnp.where(within == EDGE - 1, plus[2] * hold[5], zero),
            )
            coef[j, Q, h] = q
            coef[j, INV, h] = inverse
            power = q
            for _ in range(sh.span.bit_length() - 1):
                power = power * power
            whole = power
            for _ in range(sh.chips.bit_length() - 1):
                whole = whole * whole
            weight = 1.0 / (1.0 - ALPHA_SCALE * whole)
            for back in range(1, sh.chips + 1):
                wrapped = jnp.where(chip < back, ALPHA_SCALE, 1.0)
                coef[j, K0 + back - 1, h] = weight * wrapped
                weight = weight * power
            for d in range(COMPONENTS):
                first[j, d, h] = tiles[4 + d, slot, h]
        return 0

    lax.fori_loop(0, sh.half, step, 0)


def assemble(sh, flags, whole, other, field, rows):
    core = flags[CORE]

    def step(k, _):
        j, comp = k // COMPONENTS, k % COMPONENTS
        slot = core * sh.half + j
        for part, source in enumerate((whole, other)):
            first = (core if part == 0 else 1 - core) * sh.local

            def write(i, h, value, first=first):
                field[j, comp, first + i, h] = value

            rows_to_tiles(
                lambda c, source=source: source[slot, comp, :, c * LANES : (c + 1) * LANES],
                sh.local,
                rows.at[part],
                write,
            )
        return 0

    lax.fori_loop(0, sh.half * COMPONENTS, step, 0)


def gather_kernel(sh, flags, whole, other, field, last, *rest):
    assemble(sh, flags, whole, other, field, rest[-1])

    def step(k, _):
        j, comp = k // COMPONENTS, k % COMPONENTS
        last[j, comp] = field[j, comp, sh.span - 1]
        return 0

    lax.fori_loop(0, sh.half * COMPONENTS, step, 0)
    pack_faces(sh, flags, lambda j, c, l, h: field[j, c, l, h], field, rest[:-1])


def over_tiles(sh, visit):
    for j in range(sh.half):

        def comp_step(comp, _, j=j):
            visit(j, comp)
            return 0

        lax.fori_loop(0, COMPONENTS, comp_step, 0)


def residual_inner_kernel(sh, flags, coef, field, whole, other, inner, force, rows):
    assemble(sh, flags, whole, other, force, rows)

    def visit(j, comp):
        prior = None
        for l in range(sh.span):
            total = inner_sum(sh, flags, coef, field, j, comp, l)
            now = [field[j, comp, l, h] for h in range(2)]
            for h in range(2):
                q = coef[j, Q, h]
                value = total[h] + (0.5 * q) * force[j, comp, l, h] - now[h]
                inner[j, comp, l, h] = value if prior is None else value + q * prior[h]
            prior = now

    over_tiles(sh, visit)


def residual_outer_kernel(sh, flags, coef, inner, before, first, *rest):
    faces = rest[: sh.x_count + 1]
    inner_in, z_in, scaled, partial, last, z_ghost = rest[sh.x_count + 1 :]
    place_z_ghost(flags, inner_in, z_in, z_ghost)
    chip = flags[CHIP]

    def visit(j, comp):
        live = flags[HOLD + 6 * sh.half + j].astype(F32)
        carry = [jnp.zeros((EDGE, LANES), F32)] * 2
        for l in range(sh.span):
            total = [inner[j, comp, l, h] for h in range(2)]
            if l == 0:
                for h in range(2):
                    prior = jnp.where(chip == 0, first[j, comp, h], before[j, comp, h])
                    total[h] = total[h] + coef[j, Q, h] * prior
            total = ghost_sum(sh, flags, coef, faces, z_ghost, total, j, comp, l)
            for h in range(2):
                value = total[h] * live
                scaled[j, comp, l, h] = value
                carry[h] = value + coef[j, Q, h] * carry[h]
                partial[j, comp, l, h] = carry[h]
        for h in range(2):
            last[j, comp, h] = carry[h]

    over_tiles(sh, visit)


def sweep_inner_kernel(sh, flags, coef, field, scaled, inner):
    def visit(j, comp):
        for l in range(sh.span):
            total = inner_sum(sh, flags, coef, field, j, comp, l)
            for h in range(2):
                inner[j, comp, l, h] = scaled[j, comp, l, h] + total[h]

    over_tiles(sh, visit)


def sweep_outer_kernel(sh, flags, coef, inner, *rest):
    faces = rest[: sh.x_count + 1]
    inner_in, z_in, partial, last, z_ghost = rest[sh.x_count + 1 :]
    place_z_ghost(flags, inner_in, z_in, z_ghost)

    def visit(j, comp):
        carry = [jnp.zeros((EDGE, LANES), F32)] * 2
        for l in range(sh.span):
            total = [inner[j, comp, l, h] for h in range(2)]
            total = ghost_sum(sh, flags, coef, faces, z_ghost, total, j, comp, l)
            for h in range(2):
                carry[h] = total[h] + coef[j, Q, h] * carry[h]
                partial[j, comp, l, h] = carry[h]
        for h in range(2):
            last[j, comp, h] = carry[h]

    over_tiles(sh, visit)


def incoming_slice(sh, coef, lasts, j, comp, h):
    total = coef[j, K0, h] * lasts[0][j, comp, h]
    for back in range(1, sh.chips):
        total += coef[j, K0 + back, h] * lasts[back][j, comp, h]
    return total


def close_kernel(sh, flags, coef, partial, *rest):
    lasts, (field, *messages) = rest[: sh.chips], rest[sh.chips :]
    term = {}

    def tile(j, comp, l, h):
        if l == 0:
            term[h] = incoming_slice(sh, coef, lasts, j, comp, h)
        term[h] = coef[j, Q, h] * term[h]
        value = partial[j, comp, l, h] + term[h]
        field[j, comp, l, h] = value
        return value

    pack_faces(sh, flags, tile, field, messages)


def velocity_kernel(sh, flags, whole, other, field, out, send, rows):
    core = flags[CORE]

    def step(k, _):
        j, comp = k // COMPONENTS, k % COMPONENTS
        slot = core * sh.half + j

        def keep(c, value):
            at = slice(c * LANES, (c + 1) * LANES)
            out[slot, comp, :, at] = whole[slot, comp, :, at] + value

        def pass_on(c, value):
            at = slice(c * LANES, (c + 1) * LANES)
            send[j, comp, :, at] = other[slot, comp, :, at] + value

        own, others = core * sh.local, (1 - core) * sh.local
        tiles_to_rows(lambda i, h: field[j, comp, own + i, h], sh.local, rows.at[0], keep)
        tiles_to_rows(lambda i, h: field[j, comp, others + i, h], sh.local, rows.at[1], pass_on)
        return 0

    lax.fori_loop(0, sh.half * COMPONENTS, step, 0)


def final_inner_kernel(sh, flags, coef, field, scaled, *rest):
    lasts, (inner,) = rest[: sh.chips], rest[sh.chips :]
    chip = flags[CHIP]

    def visit(j, comp):
        prior = [
            jnp.where(chip == 0, 0.0, incoming_slice(sh, coef, lasts, j, comp, h))
            for h in range(2)
        ]
        for l in range(sh.span):
            total = inner_sum(sh, flags, coef, field, j, comp, l)
            for h in range(2):
                now = field[j, comp, l, h]
                value = scaled[j, comp, l, h] + total[h] - now
                inner[j, comp, l, h] = value + coef[j, Q, h] * prior[h]
                prior[h] = now

    over_tiles(sh, visit)


def final_outer_kernel(sh, flags, coef, inner, *rest):
    faces = rest[: sh.x_count + 1]
    inner_in, z_in, out, send, z_ghost, hold, rows = rest[sh.x_count + 1 :]
    place_z_ghost(flags, inner_in, z_in, z_ghost)
    core = flags[CORE]

    def visit(j, comp):
        live = flags[HOLD + 6 * sh.half + j].astype(F32)
        for l in range(sh.span):
            total = [inner[j, comp, l, h] for h in range(2)]
            total = ghost_sum(sh, flags, coef, faces, z_ghost, total, j, comp, l)
            for h in range(2):
                hold[l, h] = total[h] * (coef[j, INV, h] * live)
        slot = core * sh.half + j

        def keep(c, value):
            out[slot, comp, :, c * LANES : (c + 1) * LANES] = value

        def pass_on(c, value):
            send[j, comp, :, c * LANES : (c + 1) * LANES] = value

        own, others = core * sh.local, (1 - core) * sh.local
        tiles_to_rows(lambda i, h: hold[own + i, h], sh.local, rows.at[0], keep)
        tiles_to_rows(lambda i, h: hold[others + i, h], sh.local, rows.at[1], pass_on)

    over_tiles(sh, visit)


def bind(kernel, sh):
    def run(*refs):
        kernel(sh, *refs)

    return run


def body(
    iterate,
    forcing,
    initial_velocity,
    viscosity,
    peclet,
    live_patch_mask,
    neighbour_holder,
    neighbour_slot,
):
    n_time, places = lax.axis_size("tm"), lax.axis_size("space")
    slots, local = iterate.shape[:2]
    sh = Shape(slots, local, n_time, places)
    half = sh.half
    t, place = lax.axis_index("tm"), lax.axis_index("space")
    core, chip = t % 2, t // 2
    velocity = iterate.transpose(0, 2, 1, 3)
    force = forcing.transpose(0, 2, 1, 3)

    velocity_other = swap_cores(velocity, n_time)
    force_other = swap_cores(force, n_time)

    def side(bits):
        return 1 - position(place, bits) % 2

    held = lax.dynamic_slice_in_dim(neighbour_holder, core * half, half, 0) >= 0
    live = lax.dynamic_slice_in_dim(live_patch_mask, core * half, half, 0)
    flags = jnp.concatenate(
        [
            jnp.stack([core, chip, side(sh.bits[0]), side(sh.bits[1])]).astype(jnp.int32),
            held.astype(jnp.int32).reshape(-1),
            live.astype(jnp.int32),
        ]
    )
    rows = pltpu.VMEM((2, CHUNKS * local, LANES), F32)
    z_ghost = pltpu.VMEM((2,) + sh.z_shape, F32)
    messages = [sh.x_shape] * sh.x_count + [sh.y_shape, sh.z_shape, sh.z_shape]

    coef, first = call(
        bind(coefficient_kernel, sh),
        flags,
        [viscosity, peclet.transpose(1, 0, 2), initial_velocity.transpose(1, 0, 2)],
        [tile_shape(half, K0 + sh.chips), sh.slice],
        [pltpu.VMEM((CHUNKS * slots, LANES), F32), pltpu.VMEM(tile_shape(7, slots), F32)],
        name="coefficients",
    )
    field, last, *out = call(
        bind(gather_kernel, sh),
        flags,
        [velocity, velocity_other],
        [sh.field, sh.slice] + messages,
        [rows],
        name="gather",
    )
    before = lax.ppermute(last, "tm", [(a, a + 2) for a in range(n_time - 2)])
    faces = exchange(sh, out, n_time, places)
    inner, _ = call(
        bind(residual_inner_kernel, sh),
        flags,
        [coef, field, force, force_other],
        [sh.field, sh.field],
        [rows],
        flops=20_000_000,
        name="residual_inner",
    )
    scaled, partial, last = call(
        bind(residual_outer_kernel, sh),
        flags,
        [coef, inner, before, first] + faces,
        [sh.field, sh.field, sh.slice],
        [z_ghost],
        name="residual_outer",
    )

    def chip_ends(last):
        return [
            lax.ppermute(last, "tm", [(a, (a + 2 * back) % n_time) for a in range(n_time)])
            for back in range(1, sh.chips)
        ] + [last]

    correction = None
    for sweep in range(SWEEPS):
        if sweep > 0:
            (inner,) = call(
                bind(sweep_inner_kernel, sh),
                flags,
                [coef, correction, scaled],
                [sh.field],
                flops=20_000_000,
                name="sweep_inner",
            )
            partial, last = call(
                bind(sweep_outer_kernel, sh),
                flags,
                [coef, inner] + faces,
                [sh.field, sh.slice],
                [z_ghost],
                name="sweep_outer",
            )
        ends = chip_ends(last)
        correction, *out = call(
            bind(close_kernel, sh),
            flags,
            [coef, partial] + ends,
            [sh.field] + messages,
            name="close",
        )
        faces = exchange(sh, out, n_time, places)
    native = (half, COMPONENTS, local, CHUNKS * LANES)
    whole = (slots,) + native[1:]

    def restore(out, send):
        other = swap_cores(send, n_time)
        start = ((1 - core) * half, 0, 0, 0)
        return lax.dynamic_update_slice(out, other, start).transpose(0, 2, 1, 3)

    (inner,) = call(
        bind(final_inner_kernel, sh),
        flags,
        [coef, correction, scaled] + ends,
        [sh.field],
        flops=20_000_000,
        name="final_inner",
    )
    out, send = call(
        bind(velocity_kernel, sh),
        flags,
        [velocity, velocity_other, correction],
        [whole, native],
        [rows],
        name="velocity",
    )
    corrected_velocity = restore(out, send)
    out, send = call(
        bind(final_outer_kernel, sh),
        flags,
        [coef, inner] + faces,
        [whole, native],
        [z_ghost, pltpu.VMEM(tile_shape(sh.span), F32), rows],
        name="final_outer",
    )
    return corrected_velocity, restore(out, send)


def solution(mesh):
    return jax.shard_map(
        body,
        mesh=mesh,
        in_specs=(
            P("space", "tm", None, None),
            P("space", "tm", None, None),
            P("space", None, None),
            P("space", None),
            P("space", None, None),
            P("space"),
            P("space", None),
            P("space", None),
        ),
        out_specs=(P("space", "tm", None, None), P("space", "tm", None, None)),
        check_vma=False,
    )
```

```python
import jax
import jax.numpy as jnp
from jax import lax
from jax.experimental import pallas as pl
from jax.experimental.pallas import tpu as pltpu
from jax.sharding import PartitionSpec as P

EDGE = 16
LANES = 128
CHUNKS = 32
COMPONENTS = 3
ALPHA_SCALE = 0.1
WINDOW_SLICES = 16
SWEEPS = 5
STREAMS = ((0, 3),)
WORK = 6_000_000
XP, XM, YP, YM, ZP, ZM, XG, YG, ZG, Q, INV, K0 = range(12)
CORE, CHIP, SIDE_X, SIDE_Y, HOLD = range(5)
F32 = jnp.float32


def iota(shape, axis):
    return lax.broadcasted_iota(jnp.int32, shape, axis)


def tile_shape(*lead):
    return lead + (2, EDGE, LANES)


def call(kernel, flags, ins, outs, scratch=(), flops=2_000_000, name=None):
    vmem = pl.BlockSpec(memory_space=pltpu.VMEM)
    return pl.pallas_call(
        kernel,
        in_specs=[pl.BlockSpec(memory_space=pltpu.SMEM)] + [vmem] * len(ins),
        out_specs=[vmem] * len(outs),
        out_shape=[jax.ShapeDtypeStruct(s, F32) for s in outs],
        scratch_shapes=list(scratch),
        compiler_params=pltpu.CompilerParams(vmem_limit_bytes=24 * 1024 * 1024),
        cost_estimate=pl.CostEstimate(flops=flops, bytes_accessed=1_000_000, transcendentals=0),
        name=name,
    )(flags, *ins)


class Shape:
    def __init__(self, slots, local, n_time, places, base, comps):
        self.base = base
        self.comps = comps
        self.slots = slots
        self.half = slots // 2
        self.local = local
        self.span = 2 * local
        self.chips = n_time // 2
        levels = places.bit_length() - 1
        self.bits = [[b for b in range(levels) if b % 3 == d] for d in range(3)]
        self.y_per = max(1, 8 // self.span)
        self.z_per = max(1, 16 // self.span)
        self.x_shape = (2 * comps, self.span * 2, LANES)
        self.y_shape = (-(-2 // self.y_per) * comps, EDGE, LANES)
        self.z_shape = tile_shape(-(-self.half // self.z_per) * comps)
        self.x_count = len(self.bits[0])
        self.field = tile_shape(self.half, comps, self.span)
        self.slice = tile_shape(self.half, comps)
        self.messages = [self.x_shape] * self.x_count + [self.y_shape, self.z_shape, self.z_shape]
        self.z_ghost = pltpu.VMEM((2,) + self.z_shape, F32)


def position(place, bits):
    if len(bits) == 1:
        return place >> bits[0] & 1
    low, high = place >> bits[0] & 1, place >> bits[1] & 1
    return 2 * high + (low ^ high)


def exchange(sh, messages, n_time, places):
    axes = ("tm", "space")
    received = []
    x_out, y_out, inner_out, z_out = messages[:-3], messages[-3], messages[-2], messages[-1]

    def pairs(bit, bits, crossed):
        table = []
        for t in range(n_time):
            for s in range(places):
                here, there = position(s, bits), position(s ^ (1 << bit), bits)
                if abs(here - there) != 1:
                    continue
                if crossed and (there > here) != (t % 2 == 1):
                    continue
                target = t ^ 1 if crossed else t
                table.append((t * places + s, target * places + (s ^ (1 << bit))))
        return table

    z_in = lax.ppermute(z_out, axes, pairs(sh.bits[2][0], sh.bits[2], True))
    x_in = [
        lax.ppermute(x_out[i], axes, pairs(bit, sh.bits[0], False))
        for i, bit in enumerate(sh.bits[0])
    ]
    y_in = lax.ppermute(y_out, axes, pairs(sh.bits[1][0], sh.bits[1], False))
    inner_in = swap_cores(inner_out, n_time)
    return x_in + [y_in, inner_in, z_in]


def swap_cores(value, n_time):
    return lax.ppermute(value, "tm", [(t, t ^ 1) for t in range(n_time)])


def over_components(sh, visit):
    if sh.comps == 1:
        visit(0)
        return

    def step(comp, _):
        visit(comp)
        return 0

    lax.fori_loop(0, sh.comps, step, 0)


def over_tiles(sh, visit):
    def all_slots(comp):
        for j in range(sh.half):
            visit(j, comp)

    over_components(sh, all_slots)


def pack_faces(sh, flags, tile, src, outs):
    core = flags[CORE]
    lane = iota((EDGE, LANES), 1)
    within, group_of_lane = lane % EDGE, lane // EDGE
    x_outs, y_out, inner_out, z_out = outs[:-3], outs[-3], outs[-2], outs[-1]
    side_y = flags[SIDE_Y]

    def pack(comp):
        for g in range(-(-sh.half // sh.z_per)):
            low = [jnp.zeros((EDGE, LANES), F32)] * 2
            high = [jnp.zeros((EDGE, LANES), F32)] * 2
            for j in range(g * sh.z_per, min(sh.half, (g + 1) * sh.z_per)):
                for l in range(sh.span):
                    index = (j % sh.z_per) * sh.span + l
                    for h in range(2):
                        value = tile(j, comp, l, h)
                        value = pltpu.roll(value, index, 1) if index else value
                        low[h] = jnp.where(within == index, value, low[h])
                        high[h] = jnp.where(within == (index + EDGE - 1) % EDGE, value, high[h])
            for h in range(2):
                inner_out[g * sh.comps + comp, h] = jnp.where(core == 1, low[h], high[h])
                z_out[g * sh.comps + comp, h] = jnp.where(core == 1, high[h], low[h])
        for number, x_out in enumerate(x_outs):
            side = flags[SIDE_X] if number == 0 else 1 - flags[SIDE_X]
            for jj in range(2):
                for l in range(sh.span):
                    for h in range(2):
                        upper = src[2 * jj + 1, comp, l, h, EDGE - 1 : EDGE, :]
                        lower = src[2 * jj, comp, l, h, 0:1, :]
                        row = slice(2 * l + h, 2 * l + h + 1)
                        x_out[jj * sh.comps + comp, row, :] = jnp.where(side == 1, upper, lower)
        for y in range(-(-2 // sh.y_per)):
            packed = jnp.zeros((EDGE, LANES), F32)
            for jj in range(y * sh.y_per, min(2, (y + 1) * sh.y_per)):
                for l in range(sh.span):
                    index = (jj % sh.y_per) * sh.span + l
                    layer = src[2 * side_y + jj, comp, l, side_y]
                    layer = pltpu.roll(layer, EDGE * index, 1) if index else layer
                    packed = jnp.where(group_of_lane == (index + 7 * side_y) % 8, layer, packed)
            packed = jnp.where(side_y == 1, pltpu.roll(packed, EDGE, 1), packed)
            y_out[y * sh.comps + comp] = packed

    over_components(sh, pack)


def inner_sum(sh, flags, coef, src, j, comp, l):
    lane = iota((EDGE, LANES), 1)
    row = iota((EDGE, LANES), 0)
    within = lane % EDGE
    hold = [flags[HOLD + j * 6 + face].astype(F32) for face in range(4)]
    tiles = [src[j, comp, l, h] for h in range(2)]
    if j // 2 == 0:
        below, above = 0.0, src[j ^ 2, comp, l, 0] * hold[3]
    else:
        below, above = src[j ^ 2, comp, l, 1] * hold[2], 0.0
    y_next = [jnp.where(lane < EDGE, tiles[1], tiles[0]), jnp.where(lane < EDGE, above, tiles[1])]
    last = lane >= LANES - EDGE
    y_back = [jnp.where(last, below, tiles[0]), jnp.where(last, tiles[0], tiles[1])]
    result = []
    for h in range(2):
        v = tiles[h]
        if j % 2 == 0:
            before, after = 0.0, src[j ^ 1, comp, l, h, 0:1, :] * hold[1]
        else:
            before, after = src[j ^ 1, comp, l, h, EDGE - 1 : EDGE, :] * hold[0], 0.0
        total = coef[j, YP, h] * pltpu.roll(y_next[h], LANES - EDGE, 1)
        total += coef[j, YM, h] * pltpu.roll(y_back[h], EDGE, 1)
        total += coef[j, ZP, h] * pltpu.roll(v, LANES - 1, 1)
        total += coef[j, ZM, h] * pltpu.roll(v, 1, 1)
        total += coef[j, XP, h] * pltpu.roll(jnp.where(row == 0, after, v), EDGE - 1, 0)
        total += coef[j, XM, h] * pltpu.roll(jnp.where(row == EDGE - 1, before, v), 1, 0)
        result.append(total)
    return result


def ghost_sum(sh, flags, coef, faces, z_ghost, total, j, comp, l):
    xs, y_in = faces[:-1], faces[-1]
    x_side, x_row = j % 2, j // 2
    y_side, y_row = j // 2, j % 2
    y_index = (y_row % sh.y_per) * sh.span + l
    z_index = (j % sh.z_per) * sh.span + l
    z_group = (j // sh.z_per) * sh.comps + comp
    outer = x_row * sh.comps + comp
    result = []
    for h in range(2):
        value = total[h]
        value += coef[j, ZG, h] * pltpu.roll(
            z_ghost[z_index % 2, z_group, h], LANES - EDGE + 1 - z_index, 1
        )
        if h == y_side:
            group = y_in[(y_row // sh.y_per) * sh.comps + comp]
            shift = ((LANES - EDGE if y_side else 0) - EDGE * y_index) % LANES
            value += coef[j, YG, h] * (pltpu.roll(group, shift, 1) if shift else group)
        row = slice(2 * l + h, 2 * l + h + 1)
        if len(xs) == 1:
            crossed = xs[0][outer, row, :]
        else:
            wanted = flags[SIDE_X] if x_side == 1 else 1 - flags[SIDE_X]
            crossed = jnp.where(wanted == 1, xs[0][outer, row, :], xs[1][outer, row, :])
        part = slice(8 * x_side, 8 * x_side + 8)
        changed = value[part] + coef[j, XG, h, part, :] * jnp.broadcast_to(crossed, (8, LANES))
        parts = [value[:8], changed] if x_side else [changed, value[8:]]
        result.append(jnp.concatenate(parts, axis=0))
    return result


def place_z_ghost(flags, inner_in, z_in, z_ghost):
    core = flags[CORE]
    odd = iota((EDGE, LANES), 1) % 2 == 1

    def step(g, _):
        for h in range(2):
            inner, outer = inner_in[g, h], z_in[g, h]
            upper = pltpu.roll(jnp.where(core == 1, outer, inner), 2 * EDGE - 2, 1)
            lower = jnp.where(core == 1, inner, outer)
            z_ghost[0, g, h] = jnp.where(odd, lower, upper)
            z_ghost[1, g, h] = jnp.where(odd, upper, lower)
        return 0

    lax.fori_loop(0, inner_in.shape[0], step, 0)


def rows_to_tiles(read, count, rows, write):
    for chunk in range(CHUNKS):
        rows[chunk * count : (chunk + 1) * count, :] = read(chunk)
    for i in range(count):
        for h in range(2):
            write(i, h, rows[pl.ds(h * count + i, EDGE, 2 * count), :])


def tiles_to_rows(tile, count, rows, write):
    for i in range(count):
        for h in range(2):
            rows[pl.ds(h * count + i, EDGE, 2 * count), :] = tile(i, h)
    for chunk in range(CHUNKS):
        write(chunk, rows[chunk * count : (chunk + 1) * count, :])


def coefficient_kernel(sh, flags, viscosity, peclet, initial, coef, first, rows, tiles):
    core = flags[CORE]
    chip = flags[CHIP]
    slots = sh.slots

    def unpack(source, kind):
        def write(i, h, value):
            tiles[kind, i, h] = value

        rows_to_tiles(lambda c: source(c), slots, rows, write)

    unpack(lambda c: viscosity[:, c * LANES : (c + 1) * LANES], 0)
    for d in range(3):
        unpack(lambda c, d=d: peclet[d, :, c * LANES : (c + 1) * LANES], 1 + d)
    for d in range(3):
        unpack(lambda c, d=d: initial[d, :, c * LANES : (c + 1) * LANES], 4 + d)

    lane = iota((EDGE, LANES), 1)
    row = iota((EDGE, LANES), 0)
    within = lane % EDGE
    zero = jnp.zeros((EDGE, LANES), F32)

    def step(j, _):
        slot = core * sh.half + j
        hold = [flags[HOLD + j * 6 + face].astype(F32) for face in range(6)]
        for h in range(2):
            nu = tiles[0, slot, h]
            inverse = 2.0 + 6.0 * nu
            q = 2.0 / inverse
            scale = nu / inverse
            plus = [scale * (1.0 - tiles[1 + d, slot, h]) for d in range(3)]
            minus = [scale * (1.0 + tiles[1 + d, slot, h]) for d in range(3)]
            for d, (upper, lower) in enumerate(((XP, XM), (YP, YM), (ZP, ZM))):
                coef[j, upper, h] = plus[d]
                coef[j, lower, h] = minus[d]
            coef[j, ZP, h] = jnp.where(within < EDGE - 1, plus[2], zero)
            coef[j, ZM, h] = jnp.where(within > 0, minus[2], zero)
            coef[j, XG, h] = jnp.where(
                row == 0,
                minus[0] * hold[0],
                jnp.where(row == EDGE - 1, plus[0] * hold[1], zero),
            )
            if h == 0:
                coef[j, YG, h] = jnp.where(lane < EDGE, minus[1] * hold[2], zero)
            else:
                coef[j, YG, h] = jnp.where(lane >= LANES - EDGE, plus[1] * hold[3], zero)
            coef[j, ZG, h] = jnp.where(
                within == 0,
                minus[2] * hold[4],
                jnp.where(within == EDGE - 1, plus[2] * hold[5], zero),
            )
            coef[j, Q, h] = q
            coef[j, INV, h] = inverse
            power = q
            for _ in range(sh.span.bit_length() - 1):
                power = power * power
            whole = power
            for _ in range(sh.chips.bit_length() - 1):
                whole = whole * whole
            weight = 1.0 / (1.0 - ALPHA_SCALE * whole)
            for back in range(1, sh.chips + 1):
                wrapped = jnp.where(chip < back, ALPHA_SCALE, 1.0)
                coef[j, K0 + back - 1, h] = weight * wrapped
                weight = weight * power
            for d in range(COMPONENTS):
                first[j, d, h] = tiles[4 + d, slot, h]
        return 0

    lax.fori_loop(0, sh.half, step, 0)


def assemble(sh, flags, whole, other, field, rows):
    core = flags[CORE]

    def visit(j, comp):
        slot = core * sh.half + j
        for part, source in enumerate((whole, other)):
            first = (core if part == 0 else 1 - core) * sh.local

            def read(c, source=source):
                return source[slot, sh.base + comp, :, c * LANES : (c + 1) * LANES]

            def write(i, h, value, first=first):
                field[j, comp, first + i, h] = value

            rows_to_tiles(read, sh.local, rows.at[2 * j + part], write)

    over_tiles(sh, visit)


def gather_kernel(sh, flags, whole, other, field, last, *rest):
    assemble(sh, flags, whole, other, field, rest[-1])

    def visit(j, comp):
        last[j, comp] = field[j, comp, sh.span - 1]

    over_tiles(sh, visit)
    pack_faces(sh, flags, lambda j, c, l, h: field[j, c, l, h], field, rest[:-1])


def residual_inner_kernel(sh, flags, coef, field, whole, other, inner, force, rows):
    assemble(sh, flags, whole, other, force, rows)

    def visit(j, comp):
        prior = None
        for l in range(sh.span):
            total = inner_sum(sh, flags, coef, field, j, comp, l)
            now = [field[j, comp, l, h] for h in range(2)]
            for h in range(2):
                q = coef[j, Q, h]
                value = total[h] + (0.5 * q) * force[j, comp, l, h] - now[h]
                inner[j, comp, l, h] = value if prior is None else value + q * prior[h]
            prior = now

    over_tiles(sh, visit)


def residual_outer_kernel(sh, flags, coef, inner, before, first, *rest):
    faces = rest[: sh.x_count + 1]
    inner_in, z_in, scaled, partial, last, z_ghost = rest[sh.x_count + 1 :]
    place_z_ghost(flags, inner_in, z_in, z_ghost)
    chip = flags[CHIP]

    def visit(j, comp):
        live = flags[HOLD + 6 * sh.half + j].astype(F32)
        carry = [jnp.zeros((EDGE, LANES), F32)] * 2
        for l in range(sh.span):
            total = [inner[j, comp, l, h] for h in range(2)]
            if l == 0:
                for h in range(2):
                    prior = jnp.where(chip == 0, first[j, sh.base + comp, h], before[j, comp, h])
                    total[h] = total[h] + coef[j, Q, h] * prior
            total = ghost_sum(sh, flags, coef, faces, z_ghost, total, j, comp, l)
            for h in range(2):
                value = total[h] * live
                scaled[j, comp, l, h] = value
                carry[h] = value + coef[j, Q, h] * carry[h]
                partial[j, comp, l, h] = carry[h]
        for h in range(2):
            last[j, comp, h] = carry[h]

    over_tiles(sh, visit)


def sweep_inner_kernel(sh, flags, coef, field, scaled, inner):
    def visit(j, comp):
        for l in range(sh.span):
            total = inner_sum(sh, flags, coef, field, j, comp, l)
            for h in range(2):
                inner[j, comp, l, h] = scaled[j, comp, l, h] + total[h]

    over_tiles(sh, visit)


def sweep_outer_kernel(sh, flags, coef, inner, *rest):
    faces = rest[: sh.x_count + 1]
    inner_in, z_in, partial, last, z_ghost = rest[sh.x_count + 1 :]
    place_z_ghost(flags, inner_in, z_in, z_ghost)

    def visit(j, comp):
        carry = [jnp.zeros((EDGE, LANES), F32)] * 2
        for l in range(sh.span):
            total = [inner[j, comp, l, h] for h in range(2)]
            total = ghost_sum(sh, flags, coef, faces, z_ghost, total, j, comp, l)
            for h in range(2):
                carry[h] = total[h] + coef[j, Q, h] * carry[h]
                partial[j, comp, l, h] = carry[h]
        for h in range(2):
            last[j, comp, h] = carry[h]

    over_tiles(sh, visit)


def incoming_slice(sh, coef, lasts, j, comp, h):
    total = coef[j, K0, h] * lasts[0][j, comp, h]
    for back in range(1, sh.chips):
        total += coef[j, K0 + back, h] * lasts[back][j, comp, h]
    return total


def close_kernel(sh, flags, coef, partial, *rest):
    lasts, (field, *messages) = rest[: sh.chips], rest[sh.chips :]
    term = {}

    def tile(j, comp, l, h):
        if l == 0:
            term[h] = incoming_slice(sh, coef, lasts, j, comp, h)
        term[h] = coef[j, Q, h] * term[h]
        value = partial[j, comp, l, h] + term[h]
        field[j, comp, l, h] = value
        return value

    pack_faces(sh, flags, tile, field, messages)


def store_rows(sh, core, j, tile, keep, pass_on, rows):
    own, others = core * sh.local, (1 - core) * sh.local
    tiles_to_rows(lambda i, h: tile(own + i, h), sh.local, rows.at[2 * j], keep)
    tiles_to_rows(lambda i, h: tile(others + i, h), sh.local, rows.at[2 * j + 1], pass_on)


def velocity_kernel(shapes, flags, whole, other, *rest):
    core = flags[CORE]
    fields, (out, send, rows) = rest[: len(shapes)], rest[len(shapes) :]
    for sh, field in zip(shapes, fields):

        def visit(j, comp, sh=sh, field=field):
            slot = core * sh.half + j

            def keep(c, value):
                at = slice(c * LANES, (c + 1) * LANES)
                out[slot, sh.base + comp, :, at] = whole[slot, sh.base + comp, :, at] + value

            def pass_on(c, value):
                at = slice(c * LANES, (c + 1) * LANES)
                send[j, sh.base + comp, :, at] = other[slot, sh.base + comp, :, at] + value

            store_rows(sh, core, j, lambda l, h: field[j, comp, l, h], keep, pass_on, rows)

        over_tiles(sh, visit)


def final_inner_kernel(sh, flags, coef, field, scaled, *rest):
    lasts, (inner,) = rest[: sh.chips], rest[sh.chips :]
    chip = flags[CHIP]

    def visit(j, comp):
        prior = [
            jnp.where(chip == 0, 0.0, incoming_slice(sh, coef, lasts, j, comp, h))
            for h in range(2)
        ]
        for l in range(sh.span):
            total = inner_sum(sh, flags, coef, field, j, comp, l)
            for h in range(2):
                now = field[j, comp, l, h]
                value = scaled[j, comp, l, h] + total[h] - now
                inner[j, comp, l, h] = value + coef[j, Q, h] * prior[h]
                prior[h] = now

    over_tiles(sh, visit)


def final_outer_kernel(shapes, flags, coef, *rest):
    core = flags[CORE]
    count = shapes[0].x_count + 4
    ins, rest = rest[: count * len(shapes)], rest[count * len(shapes) :]
    out, send, hold, rows, *ghosts = rest
    for number, (sh, z_ghost) in enumerate(zip(shapes, ghosts)):
        inner, *faces = ins[number * count : (number + 1) * count]
        faces, inner_in, z_in = faces[:-2], faces[-2], faces[-1]
        place_z_ghost(flags, inner_in, z_in, z_ghost)

        def visit(j, comp, sh=sh, z_ghost=z_ghost, inner=inner, faces=faces):
            live = flags[HOLD + 6 * sh.half + j].astype(F32)
            for l in range(sh.span):
                total = [inner[j, comp, l, h] for h in range(2)]
                total = ghost_sum(sh, flags, coef, faces, z_ghost, total, j, comp, l)
                for h in range(2):
                    hold[j, l, h] = total[h] * (coef[j, INV, h] * live)
            slot = core * sh.half + j

            def keep(c, value):
                out[slot, sh.base + comp, :, c * LANES : (c + 1) * LANES] = value

            def pass_on(c, value):
                send[j, sh.base + comp, :, c * LANES : (c + 1) * LANES] = value

            store_rows(sh, core, j, lambda l, h: hold[j, l, h], keep, pass_on, rows)

        over_tiles(sh, visit)


def bind(kernel, sh):
    def run(*refs):
        kernel(sh, *refs)

    return run


def body(
    iterate,
    forcing,
    initial_velocity,
    viscosity,
    peclet,
    live_patch_mask,
    neighbour_holder,
    neighbour_slot,
):
    n_time, places = lax.axis_size("tm"), lax.axis_size("space")
    slots, local = iterate.shape[:2]
    shapes = [Shape(slots, local, n_time, places, base, comps) for base, comps in STREAMS]
    sh = shapes[0]
    half = sh.half
    t, place = lax.axis_index("tm"), lax.axis_index("space")
    core, chip = t % 2, t // 2
    velocity = iterate.transpose(0, 2, 1, 3)
    force = forcing.transpose(0, 2, 1, 3)

    velocity_other = swap_cores(velocity, n_time)
    force_other = swap_cores(force, n_time)

    def side(bits):
        return 1 - position(place, bits) % 2

    held = lax.dynamic_slice_in_dim(neighbour_holder, core * half, half, 0) >= 0
    live = lax.dynamic_slice_in_dim(live_patch_mask, core * half, half, 0)
    flags = jnp.concatenate(
        [
            jnp.stack([core, chip, side(sh.bits[0]), side(sh.bits[1])]).astype(jnp.int32),
            held.astype(jnp.int32).reshape(-1),
            live.astype(jnp.int32),
        ]
    )
    rows = pltpu.VMEM((2 * half, CHUNKS * local, LANES), F32)

    coef, first = call(
        bind(coefficient_kernel, sh),
        flags,
        [viscosity, peclet.transpose(1, 0, 2), initial_velocity.transpose(1, 0, 2)],
        [tile_shape(half, K0 + sh.chips), tile_shape(half, COMPONENTS)],
        [pltpu.VMEM((CHUNKS * slots, LANES), F32), pltpu.VMEM(tile_shape(7, slots), F32)],
        name="coefficients",
    )
    fields, faces, befores = [], [], []
    for sh in shapes:
        field, last, *out = call(
            bind(gather_kernel, sh),
            flags,
            [velocity, velocity_other],
            [sh.field, sh.slice] + sh.messages,
            [rows],
            name="gather",
        )
        befores.append(lax.ppermute(last, "tm", [(a, a + 2) for a in range(n_time - 2)]))
        faces.append(exchange(sh, out, n_time, places))
        fields.append(field)

    def chip_ends(sh, last):
        return [
            lax.ppermute(last, "tm", [(a, (a + 2 * back) % n_time) for a in range(n_time)])
            for back in range(1, sh.chips)
        ] + [last]

    scaleds, partials, ends = [], [], []
    for sh, field, before, face in zip(shapes, fields, befores, faces):
        inner, _ = call(
            bind(residual_inner_kernel, sh),
            flags,
            [coef, field, force, force_other],
            [sh.field, sh.field],
            [rows],
            flops=sh.comps * WORK,
            name="residual_inner",
        )
        scaled, partial, last = call(
            bind(residual_outer_kernel, sh),
            flags,
            [coef, inner, before, first] + face,
            [sh.field, sh.field, sh.slice],
            [sh.z_ghost],
            flops=sh.comps * WORK,
            name="residual_outer",
        )
        scaleds.append(scaled)
        partials.append(partial)
        ends.append(chip_ends(sh, last))

    corrections = [None] * len(shapes)
    for sweep in range(SWEEPS):
        for number, sh in enumerate(shapes):
            if sweep > 0:
                (inner,) = call(
                    bind(sweep_inner_kernel, sh),
                    flags,
                    [coef, corrections[number], scaleds[number]],
                    [sh.field],
                    flops=sh.comps * WORK,
                    name="sweep_inner",
                )
                partials[number], last = call(
                    bind(sweep_outer_kernel, sh),
                    flags,
                    [coef, inner] + faces[number],
                    [sh.field, sh.slice],
                    [sh.z_ghost],
                    flops=sh.comps * WORK,
                    name="sweep_outer",
                )
                ends[number] = chip_ends(sh, last)
            corrections[number], *out = call(
                bind(close_kernel, sh),
                flags,
                [coef, partials[number]] + ends[number],
                [sh.field] + sh.messages,
                flops=sh.comps * WORK,
                name="close",
            )
            faces[number] = exchange(sh, out, n_time, places)
    native = (half, COMPONENTS, local, CHUNKS * LANES)
    whole = (slots,) + native[1:]

    def restore(out, send):
        other = swap_cores(send, n_time)
        start = ((1 - core) * half, 0, 0, 0)
        return lax.dynamic_update_slice(out, other, start).transpose(0, 2, 1, 3)

    ins = []
    for number, sh in enumerate(shapes):
        ins += call(
            bind(final_inner_kernel, sh),
            flags,
            [coef, corrections[number], scaleds[number]] + ends[number],
            [sh.field],
            flops=sh.comps * WORK,
            name="final_inner",
        )
        ins += faces[number]
    out, send = call(
        bind(velocity_kernel, shapes),
        flags,
        [velocity, velocity_other] + corrections,
        [whole, native],
        [rows],
        flops=WORK,
        name="velocity",
    )
    corrected_velocity = restore(out, send)
    out, send = call(
        bind(final_outer_kernel, shapes),
        flags,
        [coef] + ins,
        [whole, native],
        [pltpu.VMEM(tile_shape(half, sh.span), F32), rows] + [sh.z_ghost for sh in shapes],
        name="final_outer",
    )
    return corrected_velocity, restore(out, send)


def solution(mesh):
    return jax.shard_map(
        body,
        mesh=mesh,
        in_specs=(
            P("space", "tm", None, None),
            P("space", "tm", None, None),
            P("space", None, None),
            P("space", None),
            P("space", None, None),
            P("space"),
            P("space", None),
            P("space", None),
        ),
        out_specs=(P("space", "tm", None, None), P("space", "tm", None, None)),
        check_vma=False,
    )
```

```python
import jax
import jax.numpy as jnp
from jax import lax
from jax.experimental import pallas as pl
from jax.experimental.pallas import tpu as pltpu
from jax.sharding import PartitionSpec as P


EDGE = 16
LANES = 128
CHUNKS = 32
COMPONENTS = 3
ALPHA_SCALE = 0.1
SWEEPS = 5
STREAMS = ((0, 3),)
WORK = 6_000_000
XP, XM, YP, YM, ZP, ZM, XG, YG, ZG, Q, INV, LIVE, K0 = range(13)
FACES = 6
F32 = jnp.float32


def iota(shape, axis):
    return lax.broadcasted_iota(jnp.int32, shape, axis)


def tile_shape(*lead):
    return lead + (2, EDGE, LANES)


def call(kernel, tables, ins, outs, scratch=(), flops=2_000_000, in_hbm=None):
    vmem = pl.BlockSpec(memory_space=pltpu.VMEM)
    tables = tables or []
    return pl.pallas_call(
        kernel,
        in_specs=[pl.BlockSpec(memory_space=pltpu.SMEM)] * len(tables) + [vmem] * len(ins),
        out_specs=[vmem if s != in_hbm else pl.BlockSpec(memory_space=pltpu.HBM) for s in outs],
        out_shape=[jax.ShapeDtypeStruct(s, F32) for s in outs],
        scratch_shapes=list(scratch),
        compiler_params=pltpu.CompilerParams(vmem_limit_bytes=24 * 1024 * 1024),
        cost_estimate=pl.CostEstimate(flops=flops, bytes_accessed=1_000_000, transcendentals=0),
    )(*tables, *ins)


class Shape:
    def __init__(self, slots, local, n_time, places, base, comps):
        self.base = base
        self.comps = comps
        self.slots = slots
        self.half = slots // 2
        self.local = local
        self.span = 2 * local
        self.chips = n_time // 2
        levels = places.bit_length() - 1
        self.bits = [[b for b in range(levels) if b % 3 == d] for d in range(3)]
        self.y_per = max(1, 8 // self.span)
        self.z_per = max(1, 16 // self.span)
        self.x_shape = (2 * comps, self.span * 2, LANES)
        self.y_shape = (-(-2 // self.y_per) * comps, EDGE, LANES)
        self.z_shape = tile_shape(-(-self.half // self.z_per) * comps)
        self.x_count = len(self.bits[0])
        self.field = tile_shape(self.half, comps, self.span)
        self.slice = tile_shape(self.half, comps)
        self.messages = [self.x_shape] * self.x_count + [self.y_shape, self.z_shape, self.z_shape]
        self.z_ghost = pltpu.VMEM((2,) + self.z_shape, F32)


    def core(self):
        return lax.axis_index("tm") & 1

    def upper(self):
        return self.core() ^ (position(lax.axis_index("space"), self.bits[2]) & 1)

    def chip(self):
        return lax.axis_index("tm") >> 1

    def side(self, d):
        return 1 - (position(lax.axis_index("space"), self.bits[d]) & 1)


def position(place, bits):
    if len(bits) == 1:
        return place >> bits[0] & 1
    low, high = place >> bits[0] & 1, place >> bits[1] & 1
    return 2 * high + (low ^ high)


def exchange(sh, messages, n_time, places):
    axes = ("tm", "space")
    x_out, y_out, inner_out, z_out = messages[:-3], messages[-3], messages[-2], messages[-1]

    def pairs(bit, bits, halved):
        table = []
        for t in range(n_time):
            for s in range(places):
                here, there = position(s, bits), position(s ^ (1 << bit), bits)
                if abs(here - there) != 1:
                    continue
                if halved and (min(here, there) % 2 == 0) != (t % 2 == 1):
                    continue
                table.append((t * places + s, t * places + (s ^ (1 << bit))))
        return table

    z_in = lax.ppermute(z_out, axes, pairs(sh.bits[2][0], sh.bits[2], True))
    x_in = []
    for i, bit in enumerate(sh.bits[0]):
        x_in.append(lax.ppermute(x_out[i], axes, pairs(bit, sh.bits[0], False)))
    y_in = lax.ppermute(y_out, axes, pairs(sh.bits[1][0], sh.bits[1], False))
    inner_in = swap_cores(inner_out, n_time)
    return x_in + [y_in, inner_in, z_in]


def swap_cores(value, n_time):
    return lax.ppermute(value, "tm", [(t, t ^ 1) for t in range(n_time)])


def over_components(sh, visit):
    if sh.comps == 1:
        visit(0)
        return

    def step(comp, _):
        visit(comp)
        return 0

    lax.fori_loop(0, sh.comps, step, 0)


def over_tiles(sh, visit):
    def all_slots(comp):
        for j in range(sh.half):
            visit(j, comp)

    over_components(sh, all_slots)


def pack_faces(sh, tile, src, outs):
    on_top = sh.upper()
    lane = iota((EDGE, LANES), 1)
    within, group_of_lane = lane % EDGE, lane // EDGE
    x_outs, y_out, inner_out, z_out = outs[:-3], outs[-3], outs[-2], outs[-1]
    side_y = sh.side(1)

    def pack(comp):
        for g in range(-(-sh.half // sh.z_per)):
            low = [jnp.zeros((EDGE, LANES), F32)] * 2
            high = [jnp.zeros((EDGE, LANES), F32)] * 2
            for j in range(g * sh.z_per, min(sh.half, (g + 1) * sh.z_per)):
                for l in range(sh.span):
                    index = (j % sh.z_per) * sh.span + l
                    for h in range(2):
                        value = tile(j, comp, l, h)
                        value = pltpu.roll(value, index, 1) if index else value
                        low[h] = jnp.where(within == index, value, low[h])
                        high[h] = jnp.where(within == (index + EDGE - 1) % EDGE, value, high[h])
            for h in range(2):
                inner_out[g * sh.comps + comp, h] = jnp.where(on_top == 1, low[h], high[h])
                z_out[g * sh.comps + comp, h] = jnp.where(on_top == 1, high[h], low[h])
        for number, x_out in enumerate(x_outs):
            side = sh.side(0) if number == 0 else 1 - sh.side(0)
            for jj in range(2):
                for l in range(sh.span):
                    for h in range(2):
                        upper = src[2 * jj + 1, comp, l, h, EDGE - 1 : EDGE, :]
                        lower = src[2 * jj, comp, l, h, 0:1, :]
                        row = slice(2 * l + h, 2 * l + h + 1)
                        x_out[jj * sh.comps + comp, row, :] = jnp.where(side == 1, upper, lower)
        for y in range(-(-2 // sh.y_per)):
            packed = jnp.zeros((EDGE, LANES), F32)
            for jj in range(y * sh.y_per, min(2, (y + 1) * sh.y_per)):
                for l in range(sh.span):
                    index = (jj % sh.y_per) * sh.span + l
                    layer = src[2 * side_y + jj, comp, l, side_y]
                    layer = pltpu.roll(layer, EDGE * index, 1) if index else layer
                    packed = jnp.where(group_of_lane == (index + 7 * side_y) % 8, layer, packed)
            packed = jnp.where(side_y == 1, pltpu.roll(packed, EDGE, 1), packed)
            y_out[y * sh.comps + comp] = packed

    over_components(sh, pack)


def inner_sum(coef, src, j, comp, l):
    lane = iota((EDGE, LANES), 1)
    row = iota((EDGE, LANES), 0)
    tiles = [src[j, comp, l, h] for h in range(2)]
    if j // 2 == 0:
        below, above = 0.0, src[j ^ 2, comp, l, 0]
    else:
        below, above = src[j ^ 2, comp, l, 1], 0.0
    y_next = [jnp.where(lane < EDGE, tiles[1], tiles[0]), jnp.where(lane < EDGE, above, tiles[1])]
    last = lane >= LANES - EDGE
    y_back = [jnp.where(last, below, tiles[0]), jnp.where(last, tiles[0], tiles[1])]
    result = []
    for h in range(2):
        v = tiles[h]
        if j % 2 == 0:
            before, after = 0.0, src[j ^ 1, comp, l, h, 0:1, :]
        else:
            before, after = src[j ^ 1, comp, l, h, EDGE - 1 : EDGE, :], 0.0
        total = coef[j, YP, h] * pltpu.roll(y_next[h], LANES - EDGE, 1)
        total += coef[j, YM, h] * pltpu.roll(y_back[h], EDGE, 1)
        total += coef[j, ZP, h] * pltpu.roll(v, LANES - 1, 1)
        total += coef[j, ZM, h] * pltpu.roll(v, 1, 1)
        total += coef[j, XP, h] * pltpu.roll(jnp.where(row == 0, after, v), EDGE - 1, 0)
        total += coef[j, XM, h] * pltpu.roll(jnp.where(row == EDGE - 1, before, v), 1, 0)
        result.append(total)
    return result


def ghost_sum(sh, coef, faces, z_ghost, total, j, comp, l):
    xs, y_in = faces[:-1], faces[-1]
    x_side, x_row = j % 2, j // 2
    y_side, y_row = j // 2, j % 2
    y_index = (y_row % sh.y_per) * sh.span + l
    z_index = (j % sh.z_per) * sh.span + l
    z_group = (j // sh.z_per) * sh.comps + comp
    outer = x_row * sh.comps + comp
    result = []
    for h in range(2):
        value = total[h]
        value += coef[j, ZG, h] * pltpu.roll(
            z_ghost[z_index % 2, z_group, h], LANES - EDGE + 1 - z_index, 1
        )
        if h == y_side:
            group = y_in[(y_row // sh.y_per) * sh.comps + comp]
            shift = ((LANES - EDGE if y_side else 0) - EDGE * y_index) % LANES
            value += coef[j, YG, h] * (pltpu.roll(group, shift, 1) if shift else group)
        row = slice(2 * l + h, 2 * l + h + 1)
        if len(xs) == 1:
            crossed = xs[0][outer, row, :]
        else:
            wanted = sh.side(0) if x_side == 1 else 1 - sh.side(0)
            crossed = jnp.where(wanted == 1, xs[0][outer, row, :], xs[1][outer, row, :])
        part = slice(8 * x_side, 8 * x_side + 8)
        changed = value[part] + coef[j, XG, h, part, :] * jnp.broadcast_to(crossed, (8, LANES))
        parts = [value[:8], changed] if x_side else [changed, value[8:]]
        result.append(jnp.concatenate(parts, axis=0))
    return result


def place_z_ghost(sh, inner_in, z_in, z_ghost):
    upper = sh.upper()
    odd = iota((EDGE, LANES), 1) % 2 == 1

    def step(g, _):
        for h in range(2):
            inner, outer = inner_in[g, h], z_in[g, h]
            above = pltpu.roll(jnp.where(upper == 1, outer, inner), 2 * EDGE - 2, 1)
            below = jnp.where(upper == 1, inner, outer)
            z_ghost[0, g, h] = jnp.where(odd, below, above)
            z_ghost[1, g, h] = jnp.where(odd, above, below)
        return 0

    lax.fori_loop(0, inner_in.shape[0], step, 0)


def rows_to_tiles(read, count, rows, write):
    for chunk in range(CHUNKS):
        rows[chunk * count : (chunk + 1) * count, :] = read(chunk)
    for i in range(count):
        for h in range(2):
            write(i, h, rows[pl.ds(h * count + i, EDGE, 2 * count), :])


def tiles_to_rows(tile, count, rows, write):
    for i in range(count):
        for h in range(2):
            rows[pl.ds(h * count + i, EDGE, 2 * count), :] = tile(i, h)
    for chunk in range(CHUNKS):
        write(chunk, rows[chunk * count : (chunk + 1) * count, :])


def present(holder, slot, face):
    return jnp.where(holder[slot, face] >= 0, 1.0, 0.0).astype(F32)


def coefficient_kernel(sh, holder, mask, viscosity, peclet, initial, coef, first, rows, tiles):
    chip = sh.chip()
    slots = sh.slots

    def unpack(source, kind):
        def write(i, h, value):
            tiles[kind, i, h] = value

        rows_to_tiles(lambda c: source(c), slots, rows, write)

    unpack(lambda c: viscosity[:, c * LANES : (c + 1) * LANES], 0)
    for d in range(3):
        unpack(lambda c, d=d: peclet[d, :, c * LANES : (c + 1) * LANES], 1 + d)
    for d in range(3):
        unpack(lambda c, d=d: initial[d, :, c * LANES : (c + 1) * LANES], 4 + d)

    lane = iota((EDGE, LANES), 1)
    row = iota((EDGE, LANES), 0)
    within = lane % EDGE
    zero = jnp.zeros((EDGE, LANES), F32)

    def step(j, _):
        slot = sh.upper() * sh.half + j
        hold = [present(holder, slot, face) for face in range(FACES)]
        live = mask[slot].astype(F32)
        for h in range(2):
            nu = tiles[0, slot, h]
            inverse = 2.0 + 6.0 * nu
            q = 2.0 / inverse
            scale = nu / inverse
            plus = [scale * (1.0 - tiles[1 + d, slot, h]) for d in range(3)]
            minus = [scale * (1.0 + tiles[1 + d, slot, h]) for d in range(3)]
            for d, (upper, lower) in enumerate(((XP, XM), (YP, YM), (ZP, ZM))):
                coef[j, upper, h] = plus[d]
                coef[j, lower, h] = minus[d]
            coef[j, XP, h] = jnp.where(row < EDGE - 1, plus[0], plus[0] * hold[1])
            coef[j, XM, h] = jnp.where(row > 0, minus[0], minus[0] * hold[0])
            if h == 0:
                coef[j, YM, h] = jnp.where(lane >= EDGE, minus[1], minus[1] * hold[2])
            else:
                coef[j, YP, h] = jnp.where(lane < LANES - EDGE, plus[1], plus[1] * hold[3])
            coef[j, ZP, h] = jnp.where(within < EDGE - 1, plus[2], zero)
            coef[j, ZM, h] = jnp.where(within > 0, minus[2], zero)
            coef[j, XG, h] = jnp.where(
                row == 0,
                minus[0] * hold[0],
                jnp.where(row == EDGE - 1, plus[0] * hold[1], zero),
            )
            if h == 0:
                coef[j, YG, h] = jnp.where(lane < EDGE, minus[1] * hold[2], zero)
            else:
                coef[j, YG, h] = jnp.where(lane >= LANES - EDGE, plus[1] * hold[3], zero)
            coef[j, ZG, h] = jnp.where(
                within == 0,
                minus[2] * hold[4],
                jnp.where(within == EDGE - 1, plus[2] * hold[5], zero),
            )
            coef[j, Q, h] = q
            coef[j, INV, h] = inverse * live
            coef[j, LIVE, h] = jnp.zeros_like(nu) + live
            power = q
            for _ in range(sh.span.bit_length() - 1):
                power = power * power
            whole = power
            for _ in range(sh.chips.bit_length() - 1):
                whole = whole * whole
            weight = 1.0 / (1.0 - ALPHA_SCALE * whole)
            for back in range(1, sh.chips + 1):
                wrapped = jnp.where(chip < back, ALPHA_SCALE, 1.0)
                coef[j, K0 + back - 1, h] = weight * wrapped
                weight = weight * power
            for d in range(COMPONENTS):
                first[j, d, h] = tiles[4 + d, slot, h]
        return 0

    lax.fori_loop(0, sh.half, step, 0)


def assemble(sh, whole, other, field, rows):
    core = sh.core()

    def visit(j, comp):
        slot = sh.upper() * sh.half + j
        for part, source in enumerate((whole, other)):
            first = (core if part == 0 else 1 - core) * sh.local

            def read(c, source=source):
                return source[slot, sh.base + comp, :, c * LANES : (c + 1) * LANES]

            def write(i, h, value, first=first):
                field[j, comp, first + i, h] = value

            rows_to_tiles(read, sh.local, rows.at[2 * j + part], write)

    over_tiles(sh, visit)


def gather_kernel(sh, whole, other, field, last, *rest):
    assemble(sh, whole, other, field, rest[-1])

    def visit(j, comp):
        last[j, comp] = field[j, comp, sh.span - 1]

    over_tiles(sh, visit)
    pack_faces(sh, lambda j, c, l, h: field[j, c, l, h], field, rest[:-1])


def residual_inner_kernel(sh, coef, field, whole, other, inner, force, rows):
    assemble(sh, whole, other, force, rows)

    def visit(j, comp):
        prior = None
        for l in range(sh.span):
            total = inner_sum(coef, field, j, comp, l)
            now = [field[j, comp, l, h] for h in range(2)]
            for h in range(2):
                q = coef[j, Q, h]
                value = total[h] + (0.5 * q) * force[j, comp, l, h] - now[h]
                inner[j, comp, l, h] = value if prior is None else value + q * prior[h]
            prior = now

    over_tiles(sh, visit)


def residual_outer_kernel(sh, coef, inner, before, first, *rest):
    faces = rest[: sh.x_count + 1]
    inner_in, z_in, scaled, partial, last, z_ghost = rest[sh.x_count + 1 :]
    place_z_ghost(sh, inner_in, z_in, z_ghost)
    chip = sh.chip()

    def visit(j, comp):
        carry = [jnp.zeros((EDGE, LANES), F32)] * 2
        for l in range(sh.span):
            total = [inner[j, comp, l, h] for h in range(2)]
            if l == 0:
                for h in range(2):
                    prior = jnp.where(chip == 0, first[j, sh.base + comp, h], before[j, comp, h])
                    total[h] = total[h] + coef[j, Q, h] * prior
            total = ghost_sum(sh, coef, faces, z_ghost, total, j, comp, l)
            for h in range(2):
                value = total[h] * coef[j, LIVE, h]
                scaled[j, comp, l, h] = value
                carry[h] = value + coef[j, Q, h] * carry[h]
                partial[j, comp, l, h] = carry[h]
        for h in range(2):
            last[j, comp, h] = carry[h]

    over_tiles(sh, visit)


def sweep_inner_kernel(sh, coef, field, scaled, inner):
    def visit(j, comp):
        for l in range(sh.span):
            total = inner_sum(coef, field, j, comp, l)
            for h in range(2):
                inner[j, comp, l, h] = scaled[j, comp, l, h] + total[h]

    over_tiles(sh, visit)


def sweep_outer_kernel(sh, coef, inner, *rest):
    faces = rest[: sh.x_count + 1]
    inner_in, z_in, partial, last, z_ghost = rest[sh.x_count + 1 :]
    place_z_ghost(sh, inner_in, z_in, z_ghost)

    def visit(j, comp):
        carry = [jnp.zeros((EDGE, LANES), F32)] * 2
        for l in range(sh.span):
            total = [inner[j, comp, l, h] for h in range(2)]
            total = ghost_sum(sh, coef, faces, z_ghost, total, j, comp, l)
            for h in range(2):
                carry[h] = total[h] + coef[j, Q, h] * carry[h]
                partial[j, comp, l, h] = carry[h]
        for h in range(2):
            last[j, comp, h] = carry[h]

    over_tiles(sh, visit)


def incoming_slice(sh, coef, lasts, j, comp, h):
    total = coef[j, K0, h] * lasts[0][j, comp, h]
    for back in range(1, sh.chips):
        total += coef[j, K0 + back, h] * lasts[back][j, comp, h]
    return total


def close_kernel(sh, coef, partial, *rest):
    lasts, (field, *messages) = rest[: sh.chips], rest[sh.chips :]
    term = {}

    def tile(j, comp, l, h):
        if l == 0:
            term[h] = incoming_slice(sh, coef, lasts, j, comp, h)
        term[h] = coef[j, Q, h] * term[h]
        value = partial[j, comp, l, h] + term[h]
        field[j, comp, l, h] = value
        return value

    pack_faces(sh, tile, field, messages)


def velocity_kernel(sh, whole, other, field, out, send, rows, kept, sem):
    core = sh.core()
    own, others = core * sh.local, (1 - core) * sh.local

    def visit(j, comp):
        slot = sh.upper() * sh.half + j

        def keep(c, value):
            at = slice(c * LANES, (c + 1) * LANES)
            kept[j, comp, :, at] = whole[slot, comp, :, at] + value

        def pass_on(c, value):
            at = slice(c * LANES, (c + 1) * LANES)
            send[j, comp, :, at] = other[slot, comp, :, at] + value

        tiles_to_rows(lambda i, h: field[j, comp, own + i, h], sh.local, rows.at[2 * j], keep)
        tiles_to_rows(
            lambda i, h: field[j, comp, others + i, h], sh.local, rows.at[2 * j + 1], pass_on
        )

    over_tiles(sh, visit)
    put_half(sh, sh.upper(), kept, out, sem)


def put_half(sh, which, source, out, sem):
    copy = pltpu.make_async_copy(source, out.at[pl.ds(which * sh.half, sh.half)], sem)
    copy.start()
    copy.wait()


def place_kernel(sh, half, partial, out, sem):
    put_half(sh, 1 - sh.upper(), half, out, sem)


def final_inner_kernel(sh, coef, field, scaled, *rest):
    lasts, (inner,) = rest[: sh.chips], rest[sh.chips :]
    chip = sh.chip()

    def visit(j, comp):
        prior = [
            jnp.where(chip == 0, 0.0, incoming_slice(sh, coef, lasts, j, comp, h))
            for h in range(2)
        ]
        for l in range(sh.span):
            total = inner_sum(coef, field, j, comp, l)
            for h in range(2):
                now = field[j, comp, l, h]
                value = scaled[j, comp, l, h] + total[h] - now
                inner[j, comp, l, h] = value + coef[j, Q, h] * prior[h]
                prior[h] = now

    over_tiles(sh, visit)


def final_outer_kernel(sh, mine, coef, inner, *rest):
    faces = rest[: sh.x_count + 1]
    inner_in, z_in, out, z_ghost, hold, rows, *kept = rest[sh.x_count + 1 :]
    target = kept[0] if mine else out
    place_z_ghost(sh, inner_in, z_in, z_ghost)
    core = sh.core()

    for number in range(2):

        def visit(j, comp, number=number):
            for i in range(sh.local):
                l = number * sh.local + i
                total = [inner[j, comp, l, h] for h in range(2)]
                total = ghost_sum(sh, coef, faces, z_ghost, total, j, comp, l)
                for h in range(2):
                    hold[j, i, h] = total[h] * coef[j, INV, h]

            def write(c, value):
                target[j, comp, :, c * LANES : (c + 1) * LANES] = value

            tiles_to_rows(lambda i, h: hold[j, i, h], sh.local, rows.at[j], write)

        @pl.when(core == (number if mine else 1 - number))
        def _(visit=visit):
            over_tiles(sh, visit)

    if mine:
        put_half(sh, sh.upper(), kept[0], out, kept[1])


def bind(kernel, sh, *fixed):
    def run(*refs):
        kernel(sh, *fixed, *refs)

    return run


def body(
    iterate,
    forcing,
    initial_velocity,
    viscosity,
    peclet,
    live_patch_mask,
    neighbour_holder,
    neighbour_slot,
):
    n_time, places = lax.axis_size("tm"), lax.axis_size("space")
    slots, local = iterate.shape[:2]
    shapes = [Shape(slots, local, n_time, places, base, comps) for base, comps in STREAMS]
    sh = shapes[0]
    half = sh.half
    velocity = iterate.transpose(0, 2, 1, 3)
    force = forcing.transpose(0, 2, 1, 3)

    velocity_other = swap_cores(velocity, n_time)
    force_other = swap_cores(force, n_time)

    rows = pltpu.VMEM((2 * half, CHUNKS * local, LANES), F32)

    coef, first = call(
        bind(coefficient_kernel, sh),
        [neighbour_holder, live_patch_mask],
        [viscosity, peclet.transpose(1, 0, 2), initial_velocity.transpose(1, 0, 2)],
        [tile_shape(half, K0 + sh.chips), tile_shape(half, COMPONENTS)],
        [pltpu.VMEM((CHUNKS * slots, LANES), F32), pltpu.VMEM(tile_shape(7, slots), F32)],
    )
    fields, faces, befores = [], [], []
    for sh in shapes:
        field, last, *out = call(
            bind(gather_kernel, sh),
            None,
            [velocity, velocity_other],
            [sh.field, sh.slice] + sh.messages,
            [rows],
        )
        befores.append(lax.ppermute(last, "tm", [(a, a + 2) for a in range(n_time - 2)]))
        faces.append(exchange(sh, out, n_time, places))
        fields.append(field)

    def chip_ends(sh, last):
        return [
            lax.ppermute(last, "tm", [(a, (a + 2 * back) % n_time) for a in range(n_time)])
            for back in range(1, sh.chips)
        ] + [last]

    scaleds, partials, ends = [], [], []
    for sh, field, before, face in zip(shapes, fields, befores, faces):
        inner, _ = call(
            bind(residual_inner_kernel, sh),
            None,
            [coef, field, force, force_other],
            [sh.field, sh.field],
            [rows],
            flops=sh.comps * WORK,
        )
        scaled, partial, last = call(
            bind(residual_outer_kernel, sh),
            None,
            [coef, inner, before, first] + face,
            [sh.field, sh.field, sh.slice],
            [sh.z_ghost],
            flops=sh.comps * WORK,
        )
        scaleds.append(scaled)
        partials.append(partial)
        ends.append(chip_ends(sh, last))

    corrections = [None] * len(shapes)
    for sweep in range(SWEEPS):
        for number, sh in enumerate(shapes):
            if sweep > 0:
                (inner,) = call(
                    bind(sweep_inner_kernel, sh),
                    None,
                    [coef, corrections[number], scaleds[number]],
                    [sh.field],
                    flops=sh.comps * WORK,
                )
                partials[number], last = call(
                    bind(sweep_outer_kernel, sh),
                    None,
                    [coef, inner] + faces[number],
                    [sh.field, sh.slice],
                    [sh.z_ghost],
                    flops=sh.comps * WORK,
                )
                ends[number] = chip_ends(sh, last)
            corrections[number], *out = call(
                bind(close_kernel, sh),
                None,
                [coef, partials[number]] + ends[number],
                [sh.field] + sh.messages,
                flops=sh.comps * WORK,
            )
            faces[number] = exchange(sh, out, n_time, places)
    native = (half, COMPONENTS, local, CHUNKS * LANES)
    whole = (slots,) + native[1:]

    def place(out, other):
        placed = pl.pallas_call(
            bind(place_kernel, sh),
            in_specs=[
                pl.BlockSpec(memory_space=pltpu.VMEM),
                pl.BlockSpec(memory_space=pltpu.HBM),
            ],
            out_specs=pl.BlockSpec(memory_space=pltpu.HBM),
            out_shape=jax.ShapeDtypeStruct(whole, F32),
            scratch_shapes=[pltpu.SemaphoreType.DMA(())],
            input_output_aliases={1: 0},
            name="place",
        )(other, out)
        return placed.transpose(0, 2, 1, 3)

    sh = shapes[0]
    (inner,) = call(
        bind(final_inner_kernel, sh),
        None,
        [coef, corrections[0], scaleds[0]] + ends[0],
        [sh.field],
        flops=sh.comps * WORK,
    )
    held_back, inner = lax.optimization_barrier((corrections[0], inner))
    (send,) = call(
        bind(final_outer_kernel, sh, False),
        None,
        [coef, inner] + faces[0],
        [native],
        [sh.z_ghost, pltpu.VMEM(tile_shape(half, local), F32), rows],
        flops=WORK,
    )
    residual_other = swap_cores(send, n_time)
    copied = [pltpu.VMEM(native, F32), pltpu.SemaphoreType.DMA(())]
    (residual_out,) = call(
        bind(final_outer_kernel, sh, True),
        None,
        [coef, inner] + faces[0],
        [whole],
        [sh.z_ghost, pltpu.VMEM(tile_shape(half, local), F32), rows] + copied,
        flops=WORK,
        in_hbm=whole,
    )
    out, send = call(
        bind(velocity_kernel, sh),
        None,
        [velocity, velocity_other, held_back],
        [whole, native],
        [rows] + copied,
        flops=WORK,
        in_hbm=whole,
    )
    corrected_velocity = place(out, swap_cores(send, n_time))
    return corrected_velocity, place(residual_out, residual_other)


def solution(mesh):
    return jax.shard_map(
        body,
        mesh=mesh,
        in_specs=(
            P("space", "tm", None, None),
            P("space", "tm", None, None),
            P("space", None, None),
            P("space", None),
            P("space", None, None),
            P("space"),
            P("space", None),
            P("space", None),
        ),
        out_specs=(P("space", "tm", None, None), P("space", "tm", None, None)),
        check_vma=False,
    )
```

```python
import jax
import jax.numpy as jnp
from jax import lax
from jax.experimental import pallas as pl
from jax.experimental.pallas import tpu as pltpu
from jax.sharding import PartitionSpec as P


EDGE = 16
LANES = 128
CHUNKS = 32
COMPONENTS = 3
ALPHA_SCALE = 0.1
SWEEPS = 5
STREAMS = ((0, 3),)
WORK = 6_000_000
XP, XM, YP, YM, ZP, ZM, XG, YG, ZG, Q, INV, LIVE, K0 = range(13)
FACES = 6
GRANT = 67_043_328
F32 = jnp.float32


def iota(shape, axis):
    return lax.broadcasted_iota(jnp.int32, shape, axis)


def tile_shape(*lead):
    return lead + (2, EDGE, LANES)


def call(kernel, ins, outs, scratch=(), flops=2_000_000, far=(), far_outs=(), alias=None, grant=24 << 20):
    vmem, hbm = pl.BlockSpec(memory_space=pltpu.VMEM), pl.BlockSpec(memory_space=pltpu.HBM)
    return pl.pallas_call(
        kernel,
        in_specs=[hbm if i in far else vmem for i in range(len(ins))],
        out_specs=[hbm if i in far_outs else vmem for i in range(len(outs))],
        out_shape=[jax.ShapeDtypeStruct(s, F32) for s in outs],
        scratch_shapes=list(scratch),
        input_output_aliases=alias or {},
        compiler_params=pltpu.CompilerParams(vmem_limit_bytes=grant),
        cost_estimate=pl.CostEstimate(flops=flops, bytes_accessed=1_000_000, transcendentals=0),
    )(*ins)


class Shape:
    def __init__(self, slots, local, n_time, places, base, comps):
        self.base = base
        self.comps = comps
        self.slots = slots
        self.half = slots // 2
        self.local = local
        self.span = 2 * local
        self.chips = n_time // 2
        levels = places.bit_length() - 1
        self.bits = [[b for b in range(levels) if b % 3 == d] for d in range(3)]
        self.y_per = max(1, 8 // self.span)
        self.z_per = max(1, 16 // self.span)
        self.x_shape = (2 * comps, self.span * 2, LANES)
        self.y_shape = (-(-2 // self.y_per) * comps, EDGE, LANES)
        self.z_shape = tile_shape(-(-self.half // self.z_per) * comps)
        self.x_count = len(self.bits[0])
        self.field = tile_shape(self.half, comps, self.span)
        self.slice = tile_shape(self.half, comps)
        self.messages = [self.x_shape] * self.x_count + [self.y_shape, self.z_shape, self.z_shape]
        self.z_ghost = pltpu.VMEM((2,) + self.z_shape, F32)


    def core(self):
        return lax.axis_index("tm") & 1

    def upper(self):
        return self.core() ^ (position(lax.axis_index("space"), self.bits[2]) & 1)

    def chip(self):
        return lax.axis_index("tm") >> 1

    def side(self, d):
        return 1 - (position(lax.axis_index("space"), self.bits[d]) & 1)


def position(place, bits):
    if len(bits) == 1:
        return place >> bits[0] & 1
    low, high = place >> bits[0] & 1, place >> bits[1] & 1
    return 2 * high + (low ^ high)


def exchange(sh, messages, n_time, places):
    axes = ("tm", "space")
    x_out, y_out, inner_out, z_out = messages[:-3], messages[-3], messages[-2], messages[-1]

    def pairs(bit, bits, halved):
        table = []
        for t in range(n_time):
            for s in range(places):
                here, there = position(s, bits), position(s ^ (1 << bit), bits)
                if abs(here - there) != 1:
                    continue
                if halved and (min(here, there) % 2 == 0) != (t % 2 == 1):
                    continue
                table.append((t * places + s, t * places + (s ^ (1 << bit))))
        return table

    z_in = lax.ppermute(z_out, axes, pairs(sh.bits[2][0], sh.bits[2], True))
    x_in = []
    for i, bit in enumerate(sh.bits[0]):
        x_in.append(lax.ppermute(x_out[i], axes, pairs(bit, sh.bits[0], False)))
    y_in = lax.ppermute(y_out, axes, pairs(sh.bits[1][0], sh.bits[1], False))
    inner_in = swap_cores(inner_out, n_time)
    return x_in + [y_in, inner_in, z_in]


def swap_cores(value, n_time):
    return lax.ppermute(value, "tm", [(t, t ^ 1) for t in range(n_time)])


def over_components(sh, visit):
    if sh.comps == 1:
        visit(0)
        return

    def step(comp, _):
        visit(comp)
        return 0

    lax.fori_loop(0, sh.comps, step, 0)


def over_tiles(sh, visit):
    def all_slots(comp):
        for j in range(sh.half):
            visit(j, comp)

    over_components(sh, all_slots)


def pack_faces(sh, tile, src, outs):
    on_top = sh.upper()
    lane = iota((EDGE, LANES), 1)
    within, group_of_lane = lane % EDGE, lane // EDGE
    x_outs, y_out, inner_out, z_out = outs[:-3], outs[-3], outs[-2], outs[-1]
    side_y = sh.side(1)

    def pack(comp):
        for g in range(-(-sh.half // sh.z_per)):
            low = [jnp.zeros((EDGE, LANES), F32)] * 2
            high = [jnp.zeros((EDGE, LANES), F32)] * 2
            for j in range(g * sh.z_per, min(sh.half, (g + 1) * sh.z_per)):
                for l in range(sh.span):
                    index = (j % sh.z_per) * sh.span + l
                    for h in range(2):
                        value = tile(j, comp, l, h)
                        value = pltpu.roll(value, index, 1) if index else value
                        low[h] = jnp.where(within == index, value, low[h])
                        high[h] = jnp.where(within == (index + EDGE - 1) % EDGE, value, high[h])
            for h in range(2):
                inner_out[g * sh.comps + comp, h] = jnp.where(on_top == 1, low[h], high[h])
                z_out[g * sh.comps + comp, h] = jnp.where(on_top == 1, high[h], low[h])
        for number, x_out in enumerate(x_outs):
            side = sh.side(0) if number == 0 else 1 - sh.side(0)
            for jj in range(2):
                for l in range(sh.span):
                    for h in range(2):
                        upper = src[2 * jj + 1, comp, l, h, EDGE - 1 : EDGE, :]
                        lower = src[2 * jj, comp, l, h, 0:1, :]
                        row = slice(2 * l + h, 2 * l + h + 1)
                        x_out[jj * sh.comps + comp, row, :] = jnp.where(side == 1, upper, lower)
        for y in range(-(-2 // sh.y_per)):
            packed = jnp.zeros((EDGE, LANES), F32)
            for jj in range(y * sh.y_per, min(2, (y + 1) * sh.y_per)):
                for l in range(sh.span):
                    index = (jj % sh.y_per) * sh.span + l
                    layer = src[2 * side_y + jj, comp, l, side_y]
                    layer = pltpu.roll(layer, EDGE * index, 1) if index else layer
                    packed = jnp.where(group_of_lane == (index + 7 * side_y) % 8, layer, packed)
            packed = jnp.where(side_y == 1, pltpu.roll(packed, EDGE, 1), packed)
            y_out[y * sh.comps + comp] = packed

    over_components(sh, pack)


def inner_sum(coef, src, j, comp, l):
    lane = iota((EDGE, LANES), 1)
    row = iota((EDGE, LANES), 0)
    tiles = [src[j, comp, l, h] for h in range(2)]
    if j // 2 == 0:
        below, above = 0.0, src[j ^ 2, comp, l, 0]
    else:
        below, above = src[j ^ 2, comp, l, 1], 0.0
    y_next = [jnp.where(lane < EDGE, tiles[1], tiles[0]), jnp.where(lane < EDGE, above, tiles[1])]
    last = lane >= LANES - EDGE
    y_back = [jnp.where(last, below, tiles[0]), jnp.where(last, tiles[0], tiles[1])]
    result = []
    for h in range(2):
        v = tiles[h]
        if j % 2 == 0:
            before, after = 0.0, src[j ^ 1, comp, l, h, 0:1, :]
        else:
            before, after = src[j ^ 1, comp, l, h, EDGE - 1 : EDGE, :], 0.0
        total = coef[j, YP, h] * pltpu.roll(y_next[h], LANES - EDGE, 1)
        total += coef[j, YM, h] * pltpu.roll(y_back[h], EDGE, 1)
        total += coef[j, ZP, h] * pltpu.roll(v, LANES - 1, 1)
        total += coef[j, ZM, h] * pltpu.roll(v, 1, 1)
        total += coef[j, XP, h] * pltpu.roll(jnp.where(row == 0, after, v), EDGE - 1, 0)
        total += coef[j, XM, h] * pltpu.roll(jnp.where(row == EDGE - 1, before, v), 1, 0)
        result.append(total)
    return result


def ghost_sum(sh, coef, faces, z_ghost, total, j, comp, l):
    xs, y_in = faces[:-1], faces[-1]
    x_side, x_row = j % 2, j // 2
    y_side, y_row = j // 2, j % 2
    y_index = (y_row % sh.y_per) * sh.span + l
    z_index = (j % sh.z_per) * sh.span + l
    z_group = (j // sh.z_per) * sh.comps + comp
    outer = x_row * sh.comps + comp
    result = []
    for h in range(2):
        value = total[h]
        value += coef[j, ZG, h] * pltpu.roll(
            z_ghost[z_index % 2, z_group, h], LANES - EDGE + 1 - z_index, 1
        )
        if h == y_side:
            group = y_in[(y_row // sh.y_per) * sh.comps + comp]
            shift = ((LANES - EDGE if y_side else 0) - EDGE * y_index) % LANES
            value += coef[j, YG, h] * (pltpu.roll(group, shift, 1) if shift else group)
        row = slice(2 * l + h, 2 * l + h + 1)
        if len(xs) == 1:
            crossed = xs[0][outer, row, :]
        else:
            wanted = sh.side(0) if x_side == 1 else 1 - sh.side(0)
            crossed = jnp.where(wanted == 1, xs[0][outer, row, :], xs[1][outer, row, :])
        part = slice(8 * x_side, 8 * x_side + 8)
        changed = value[part] + coef[j, XG, h, part, :] * jnp.broadcast_to(crossed, (8, LANES))
        parts = [value[:8], changed] if x_side else [changed, value[8:]]
        result.append(jnp.concatenate(parts, axis=0))
    return result


def place_z_ghost(sh, inner_in, z_in, z_ghost):
    upper = sh.upper()
    odd = iota((EDGE, LANES), 1) % 2 == 1

    def step(g, _):
        for h in range(2):
            inner, outer = inner_in[g, h], z_in[g, h]
            above = pltpu.roll(jnp.where(upper == 1, outer, inner), 2 * EDGE - 2, 1)
            below = jnp.where(upper == 1, inner, outer)
            z_ghost[0, g, h] = jnp.where(odd, below, above)
            z_ghost[1, g, h] = jnp.where(odd, above, below)
        return 0

    lax.fori_loop(0, inner_in.shape[0], step, 0)


def rows_to_tiles(read, count, rows, write):
    for chunk in range(CHUNKS):
        rows[chunk * count : (chunk + 1) * count, :] = read(chunk)
    for i in range(count):
        for h in range(2):
            write(i, h, rows[pl.ds(h * count + i, EDGE, 2 * count), :])


def tiles_to_rows(tile, count, rows, write):
    for i in range(count):
        for h in range(2):
            rows[pl.ds(h * count + i, EDGE, 2 * count), :] = tile(i, h)
    for chunk in range(CHUNKS):
        write(chunk, rows[chunk * count : (chunk + 1) * count, :])


def present(holder, slot, face):
    return jnp.where(holder[slot, face] >= 0, 1.0, 0.0).astype(F32)


def prepare_kernel(sh, *refs):
    far, (coef, first, own), rest = refs[:6], refs[6:9], refs[9:]
    near, (sems, rows, tiles, native_rows) = rest[:6], rest[6:]
    mine = pl.ds(sh.upper() * sh.half, sh.half)
    copies = [
        pltpu.make_async_copy(a.at[mine] if i == 5 else a, b, sems.at[i])
        for i, (a, b) in enumerate(zip(far, near))
    ]
    for copy in copies:
        copy.start()
    for copy in copies[:5]:
        copy.wait()
    coefficients(sh, *near[:5], coef, first, rows, tiles)
    copies[5].wait()
    unpack_half(sh, 0, near[5], own, 0, native_rows, 0)


def coefficients(sh, holder, mask, viscosity, peclet, initial, coef, first, rows, tiles):
    chip = sh.chip()
    slots = sh.slots

    def unpack(source, kind):
        def write(i, h, value):
            tiles[kind, i, h] = value

        rows_to_tiles(lambda c: source(c), slots, rows, write)

    unpack(lambda c: viscosity[:, c * LANES : (c + 1) * LANES], 0)
    for d in range(3):
        unpack(lambda c, d=d: peclet[d, :, c * LANES : (c + 1) * LANES], 1 + d)
    for d in range(3):
        unpack(lambda c, d=d: initial[d, :, c * LANES : (c + 1) * LANES], 4 + d)

    lane = iota((EDGE, LANES), 1)
    row = iota((EDGE, LANES), 0)
    within = lane % EDGE
    zero = jnp.zeros((EDGE, LANES), F32)

    def step(j, _):
        slot = sh.upper() * sh.half + j
        hold = [present(holder, slot, face) for face in range(FACES)]
        live = mask[slot].astype(F32)
        for h in range(2):
            nu = tiles[0, slot, h]
            inverse = 2.0 + 6.0 * nu
            q = 2.0 / inverse
            scale = nu / inverse
            plus = [scale * (1.0 - tiles[1 + d, slot, h]) for d in range(3)]
            minus = [scale * (1.0 + tiles[1 + d, slot, h]) for d in range(3)]
            for d, (upper, lower) in enumerate(((XP, XM), (YP, YM), (ZP, ZM))):
                coef[j, upper, h] = plus[d]
                coef[j, lower, h] = minus[d]
            coef[j, XP, h] = jnp.where(row < EDGE - 1, plus[0], plus[0] * hold[1])
            coef[j, XM, h] = jnp.where(row > 0, minus[0], minus[0] * hold[0])
            if h == 0:
                coef[j, YM, h] = jnp.where(lane >= EDGE, minus[1], minus[1] * hold[2])
            else:
                coef[j, YP, h] = jnp.where(lane < LANES - EDGE, plus[1], plus[1] * hold[3])
            coef[j, ZP, h] = jnp.where(within < EDGE - 1, plus[2], zero)
            coef[j, ZM, h] = jnp.where(within > 0, minus[2], zero)
            coef[j, XG, h] = jnp.where(
                row == 0,
                minus[0] * hold[0],
                jnp.where(row == EDGE - 1, plus[0] * hold[1], zero),
            )
            if h == 0:
                coef[j, YG, h] = jnp.where(lane < EDGE, minus[1] * hold[2], zero)
            else:
                coef[j, YG, h] = jnp.where(lane >= LANES - EDGE, plus[1] * hold[3], zero)
            coef[j, ZG, h] = jnp.where(
                within == 0,
                minus[2] * hold[4],
                jnp.where(within == EDGE - 1, plus[2] * hold[5], zero),
            )
            coef[j, Q, h] = q
            coef[j, INV, h] = inverse * live
            coef[j, LIVE, h] = jnp.zeros_like(nu) + live
            power = q
            for _ in range(sh.span.bit_length() - 1):
                power = power * power
            whole = power
            for _ in range(sh.chips.bit_length() - 1):
                whole = whole * whole
            weight = 1.0 / (1.0 - ALPHA_SCALE * whole)
            for back in range(1, sh.chips + 1):
                wrapped = jnp.where(chip < back, ALPHA_SCALE, 1.0)
                coef[j, K0 + back - 1, h] = weight * wrapped
                weight = weight * power
            for d in range(COMPONENTS):
                first[j, d, h] = tiles[4 + d, slot, h]
        return 0

    lax.fori_loop(0, sh.half, step, 0)


def unpack_half(sh, which, source, field, first, rows, base=None):
    def visit(j, comp):
        slot = (sh.upper() * sh.half if base is None else base) + j

        def read(c):
            return source[slot, comp, :, c * LANES : (c + 1) * LANES]

        def write(i, h, value):
            field[j, comp, first + i, h] = value

        rows_to_tiles(read, sh.local, rows.at[2 * j + which], write)

    over_tiles(sh, visit)


def gather_kernel(sh, own, other, field, last, *rest):
    core = sh.core()
    unpack_half(sh, 1, other, field, (1 - core) * sh.local, rest[-1])

    def visit(j, comp):
        for i in range(sh.local):
            for h in range(2):
                field[j, comp, core * sh.local + i, h] = own[j, comp, i, h]
        last[j, comp] = field[j, comp, sh.span - 1]

    over_tiles(sh, visit)
    pack_faces(sh, lambda j, c, l, h: field[j, c, l, h], field, rest[:-1])


def residual_inner_kernel(sh, coef, field, whole, other, inner, force, rows):
    core = sh.core()
    unpack_half(sh, 0, whole, force, core * sh.local, rows)
    unpack_half(sh, 1, other, force, (1 - core) * sh.local, rows)

    def visit(j, comp):
        prior = None
        for l in range(sh.span):
            total = inner_sum(coef, field, j, comp, l)
            now = [field[j, comp, l, h] for h in range(2)]
            for h in range(2):
                q = coef[j, Q, h]
                value = total[h] + (0.5 * q) * force[j, comp, l, h] - now[h]
                inner[j, comp, l, h] = value if prior is None else value + q * prior[h]
            prior = now

    over_tiles(sh, visit)


def residual_outer_kernel(sh, coef, inner, before, first, *rest):
    faces = rest[: sh.x_count + 1]
    inner_in, z_in, scaled, partial, last, z_ghost = rest[sh.x_count + 1 :]
    place_z_ghost(sh, inner_in, z_in, z_ghost)
    chip = sh.chip()

    def visit(j, comp):
        carry = [jnp.zeros((EDGE, LANES), F32)] * 2
        for l in range(sh.span):
            total = [inner[j, comp, l, h] for h in range(2)]
            if l == 0:
                for h in range(2):
                    prior = jnp.where(chip == 0, first[j, sh.base + comp, h], before[j, comp, h])
                    total[h] = total[h] + coef[j, Q, h] * prior
            total = ghost_sum(sh, coef, faces, z_ghost, total, j, comp, l)
            for h in range(2):
                value = total[h] * coef[j, LIVE, h]
                scaled[j, comp, l, h] = value
                carry[h] = value + coef[j, Q, h] * carry[h]
                partial[j, comp, l, h] = carry[h]
        for h in range(2):
            last[j, comp, h] = carry[h]

    over_tiles(sh, visit)


def sweep_inner_kernel(sh, coef, field, scaled, inner):
    def visit(j, comp):
        for l in range(sh.span):
            total = inner_sum(coef, field, j, comp, l)
            for h in range(2):
                inner[j, comp, l, h] = scaled[j, comp, l, h] + total[h]

    over_tiles(sh, visit)


def sweep_outer_kernel(sh, coef, inner, *rest):
    faces = rest[: sh.x_count + 1]
    inner_in, z_in, partial, last, z_ghost = rest[sh.x_count + 1 :]
    place_z_ghost(sh, inner_in, z_in, z_ghost)

    def visit(j, comp):
        carry = [jnp.zeros((EDGE, LANES), F32)] * 2
        for l in range(sh.span):
            total = [inner[j, comp, l, h] for h in range(2)]
            total = ghost_sum(sh, coef, faces, z_ghost, total, j, comp, l)
            for h in range(2):
                carry[h] = total[h] + coef[j, Q, h] * carry[h]
                partial[j, comp, l, h] = carry[h]
        for h in range(2):
            last[j, comp, h] = carry[h]

    over_tiles(sh, visit)


def incoming_slice(sh, coef, lasts, j, comp, h):
    total = coef[j, K0, h] * lasts[0][j, comp, h]
    for back in range(1, sh.chips):
        total += coef[j, K0 + back, h] * lasts[back][j, comp, h]
    return total


def close_kernel(sh, coef, partial, *rest):
    lasts, (field, *messages) = rest[: sh.chips], rest[sh.chips :]
    term = {}

    def tile(j, comp, l, h):
        if l == 0:
            term[h] = incoming_slice(sh, coef, lasts, j, comp, h)
        term[h] = coef[j, Q, h] * term[h]
        value = partial[j, comp, l, h] + term[h]
        field[j, comp, l, h] = value
        return value

    pack_faces(sh, tile, field, messages)


def velocity_kernel(sh, whole, other, field, out, send, rows, kept, sems):
    core = sh.core()
    own, others = core * sh.local, (1 - core) * sh.local

    def visit(j, comp):
        slot = sh.upper() * sh.half + j

        def keep(c, value):
            at = slice(c * LANES, (c + 1) * LANES)
            kept[j, comp, :, at] = whole[slot, comp, :, at] + value

        def pass_on(c, value):
            at = slice(c * LANES, (c + 1) * LANES)
            send[j, comp, :, at] = other[slot, comp, :, at] + value

        tiles_to_rows(lambda i, h: field[j, comp, own + i, h], sh.local, rows.at[2 * j], keep)
        tiles_to_rows(
            lambda i, h: field[j, comp, others + i, h], sh.local, rows.at[2 * j + 1], pass_on
        )

    def component(comp):
        for j in range(sh.half):
            visit(j, comp)
        put_copy(sh, comp, kept, out, sems).start()

    over_components(sh, component)
    wait_copies(sh, kept, out, sems)


def put_copy(sh, comp, kept, out, sems):
    slots = pl.ds(sh.upper() * sh.half, sh.half)
    return pltpu.make_async_copy(kept.at[:, comp], out.at[slots, comp], sems.at[comp])


def wait_copies(sh, kept, out, sems):
    for comp in range(sh.comps):
        put_copy(sh, comp, kept, out, sems).wait()


def bounce_copies(sh, comp, half, out, buffer, sems):
    slots = pl.ds((1 - sh.upper()) * sh.half, sh.half)
    first = pltpu.make_async_copy(half.at[:, comp], buffer.at[:, comp], sems.at[0, comp])
    if out is None:
        return first, None
    return first, pltpu.make_async_copy(
        buffer.at[:, comp], out.at[slots, comp], sems.at[1, comp]
    )


def start_bounce(sh, half, buffer, sems):
    for comp in range(sh.comps):
        bounce_copies(sh, comp, half, None, buffer, sems)[0].start()


def end_bounce(sh, half, out, buffer, sems):
    for comp in range(sh.comps):
        first, second = bounce_copies(sh, comp, half, out, buffer, sems)
        first.wait()
        second.start()
    for comp in range(sh.comps):
        bounce_copies(sh, comp, half, out, buffer, sems)[1].wait()


def place_kernel(sh, half, partial, out, buffer, sems):
    start_bounce(sh, half, buffer, sems)
    end_bounce(sh, half, out, buffer, sems)


def final_inner_kernel(sh, coef, field, scaled, *rest):
    lasts, (inner,) = rest[: sh.chips], rest[sh.chips :]
    chip = sh.chip()

    def visit(j, comp):
        prior = [
            jnp.where(chip == 0, 0.0, incoming_slice(sh, coef, lasts, j, comp, h))
            for h in range(2)
        ]
        for l in range(sh.span):
            total = inner_sum(coef, field, j, comp, l)
            for h in range(2):
                now = field[j, comp, l, h]
                value = scaled[j, comp, l, h] + total[h] - now
                inner[j, comp, l, h] = value + coef[j, Q, h] * prior[h]
                prior[h] = now

    over_tiles(sh, visit)


def final_outer_kernel(sh, mine, coef, inner, *rest):
    faces = rest[: sh.x_count + 1]
    if mine:
        inner_in, z_in, half, partial, out, placed, z_ghost, hold, rows, *kept = rest[sh.x_count + 1 :]
        bounce = kept[2:]
        start_bounce(sh, half, *bounce)
    else:
        inner_in, z_in, out, z_ghost, hold, rows = rest[sh.x_count + 1 :]
    target = kept[0] if mine else out
    place_z_ghost(sh, inner_in, z_in, z_ghost)
    core = sh.core()

    for number in range(2):

        def visit(j, comp, number=number):
            for i in range(sh.local):
                l = number * sh.local + i
                total = [inner[j, comp, l, h] for h in range(2)]
                total = ghost_sum(sh, coef, faces, z_ghost, total, j, comp, l)
                for h in range(2):
                    hold[j, i, h] = total[h] * coef[j, INV, h]

            def write(c, value):
                target[j, comp, :, c * LANES : (c + 1) * LANES] = value

            tiles_to_rows(lambda i, h: hold[j, i, h], sh.local, rows.at[j], write)

        def component(comp, visit=visit):
            for j in range(sh.half):
                visit(j, comp)
            if mine:
                put_copy(sh, comp, kept[0], out, kept[1]).start()

        @pl.when(core == (number if mine else 1 - number))
        def _(component=component):
            over_components(sh, component)

    if mine:
        end_bounce(sh, half, placed, *bounce)
        wait_copies(sh, kept[0], out, kept[1])


def bind(kernel, sh, *fixed):
    def run(*refs):
        kernel(sh, *fixed, *refs)

    return run


def body(
    iterate,
    forcing,
    initial_velocity,
    viscosity,
    peclet,
    live_patch_mask,
    neighbour_holder,
    neighbour_slot,
):
    n_time, places = lax.axis_size("tm"), lax.axis_size("space")
    slots, local = iterate.shape[:2]
    shapes = [Shape(slots, local, n_time, places, base, comps) for base, comps in STREAMS]
    sh = shapes[0]
    half = sh.half
    velocity = iterate.transpose(0, 2, 1, 3)
    force = forcing.transpose(0, 2, 1, 3)

    velocity_other = swap_cores(velocity, n_time)
    force_other = swap_cores(force, n_time)

    rows = pltpu.VMEM((2 * half, CHUNKS * local, LANES), F32)

    native = (half, COMPONENTS, local, CHUNKS * LANES)
    whole = (slots,) + native[1:]
    params = [
        neighbour_holder,
        live_patch_mask,
        viscosity,
        peclet.transpose(1, 0, 2),
        initial_velocity.transpose(1, 0, 2),
    ]
    near = [(pltpu.SMEM if i < 2 else pltpu.VMEM)(p.shape, p.dtype) for i, p in enumerate(params)]
    sh = shapes[0]
    coef, first, own = call(
        bind(prepare_kernel, sh),
        params + [velocity],
        [tile_shape(half, K0 + sh.chips), tile_shape(half, COMPONENTS), tile_shape(half, COMPONENTS, local)],
        near
        + [
            pltpu.VMEM(native, F32),
            pltpu.SemaphoreType.DMA((6,)),
            pltpu.VMEM((CHUNKS * slots, LANES), F32),
            pltpu.VMEM(tile_shape(7, slots), F32),
            rows,
        ],
        flops=WORK,
        far=range(6),
        grant=GRANT - velocity.size * 4 * 9 // 4,
    )
    coef, first, own, arrived = lax.optimization_barrier((coef, first, own, velocity_other))
    fields, faces, befores = [], [], []
    for sh in shapes:
        field, last, *out = call(
            bind(gather_kernel, sh), [own, arrived], [sh.field, sh.slice] + sh.messages, [rows]
        )
        befores.append(lax.ppermute(last, "tm", [(a, (a + 2) % n_time) for a in range(n_time)]))
        faces.append(exchange(sh, out, n_time, places))
        fields.append(field)

    def chip_ends(sh, last):
        return [
            lax.ppermute(last, "tm", [(a, (a + 2 * back) % n_time) for a in range(n_time)])
            for back in range(1, sh.chips)
        ] + [last]

    scaleds, partials, ends = [], [], []
    for sh, field, before, face in zip(shapes, fields, befores, faces):
        inner, _ = call(
            bind(residual_inner_kernel, sh),
            [coef, field, force, force_other],
            [sh.field, sh.field],
            [rows],
            flops=sh.comps * WORK,
        )
        scaled, partial, last = call(
            bind(residual_outer_kernel, sh),
            [coef, inner, before, first] + face,
            [sh.field, sh.field, sh.slice],
            [sh.z_ghost],
            flops=sh.comps * WORK,
        )
        scaleds.append(scaled)
        partials.append(partial)
        ends.append(chip_ends(sh, last))

    corrections = [None] * len(shapes)
    for sweep in range(SWEEPS):
        for number, sh in enumerate(shapes):
            if sweep > 0:
                (inner,) = call(
                    bind(sweep_inner_kernel, sh),
                    [coef, corrections[number], scaleds[number]],
                    [sh.field],
                    flops=sh.comps * WORK,
                )
                partials[number], last = call(
                    bind(sweep_outer_kernel, sh),
                    [coef, inner] + faces[number],
                    [sh.field, sh.slice],
                    [sh.z_ghost],
                    flops=sh.comps * WORK,
                )
                ends[number] = chip_ends(sh, last)
            corrections[number], *out = call(
                bind(close_kernel, sh),
                [coef, partials[number]] + ends[number],
                [sh.field] + sh.messages,
                flops=sh.comps * WORK,
            )
            faces[number] = exchange(sh, out, n_time, places)
    sh = shapes[0]
    (inner,) = call(
        bind(final_inner_kernel, sh),
        [coef, corrections[0], scaleds[0]] + ends[0],
        [sh.field],
        flops=sh.comps * WORK,
    )
    held_back, inner = lax.optimization_barrier((corrections[0], inner))
    copied = [pltpu.VMEM(native, F32), pltpu.SemaphoreType.DMA((COMPONENTS,))]
    bounce = [pltpu.VMEM(native, F32), pltpu.SemaphoreType.DMA((2, COMPONENTS))]
    velocity_out, send = call(
        bind(velocity_kernel, sh),
        [velocity, velocity_other, held_back],
        [whole, native],
        [rows] + copied,
        flops=WORK,
        far_outs=(0,),
    )
    velocity_other = swap_cores(send, n_time)
    (send,) = call(
        bind(final_outer_kernel, sh, False),
        [coef, inner] + faces[0],
        [native],
        [sh.z_ghost, pltpu.VMEM(tile_shape(half, local), F32), rows],
        flops=WORK,
    )
    residual_other = swap_cores(send, n_time)
    ins = [coef, inner] + faces[0] + [velocity_other, velocity_out]
    residual_out, corrected_velocity = call(
        bind(final_outer_kernel, sh, True),
        ins,
        [whole, whole],
        [sh.z_ghost, pltpu.VMEM(tile_shape(half, local), F32), rows] + copied + bounce,
        flops=WORK,
        far=(len(ins) - 2, len(ins) - 1),
        far_outs=(0, 1),
        alias={len(ins) - 1: 1},
    )
    (corrected_residual,) = call(
        bind(place_kernel, sh),
        [residual_other, residual_out],
        [whole],
        bounce,
        far=(0, 1),
        far_outs=(0,),
        alias={1: 0},
    )
    return corrected_velocity.transpose(0, 2, 1, 3), corrected_residual.transpose(0, 2, 1, 3)


def solution(mesh):
    return jax.shard_map(
        body,
        mesh=mesh,
        in_specs=(
            P("space", "tm", None, None),
            P("space", "tm", None, None),
            P("space", None, None),
            P("space", None),
            P("space", None, None),
            P("space"),
            P("space", None),
            P("space", None),
        ),
        out_specs=(P("space", "tm", None, None), P("space", "tm", None, None)),
        check_vma=False,
    )
```

```python
import jax
import jax.numpy as jnp
from jax import lax
from jax.experimental import pallas as pl
from jax.experimental.pallas import tpu as pltpu
from jax.sharding import PartitionSpec as P


EDGE = 16
LANES = 128
CHUNKS = 32
COMPONENTS = 3
ALPHA_SCALE = 0.1
SWEEPS = 5
STREAMS = ((0, 3),)
WORK = 6_000_000
XP, XM, YP, YM, ZP, ZM, XG, YG, ZG, Q, INV, LIVE, K0 = range(13)
FACES = 6
GRANT = 67_043_328
F32 = jnp.float32


def iota(shape, axis):
    return lax.broadcasted_iota(jnp.int32, shape, axis)


def tile_shape(*lead):
    return lead + (2, EDGE, LANES)


def call(kernel, ins, outs, scratch=(), flops=2_000_000, far=(), far_outs=(), alias=None, grant=24 << 20):
    vmem, hbm = pl.BlockSpec(memory_space=pltpu.VMEM), pl.BlockSpec(memory_space=pltpu.HBM)
    return pl.pallas_call(
        kernel,
        in_specs=[hbm if i in far else vmem for i in range(len(ins))],
        out_specs=[hbm if i in far_outs else vmem for i in range(len(outs))],
        out_shape=[jax.ShapeDtypeStruct(s, F32) for s in outs],
        scratch_shapes=list(scratch),
        input_output_aliases=alias or {},
        compiler_params=pltpu.CompilerParams(vmem_limit_bytes=grant),
        cost_estimate=pl.CostEstimate(flops=flops, bytes_accessed=1_000_000, transcendentals=0),
    )(*ins)


class Shape:
    def __init__(self, slots, local, n_time, places, base, comps):
        self.base = base
        self.comps = comps
        self.slots = slots
        self.half = slots // 2
        self.local = local
        self.span = 2 * local
        self.chips = n_time // 2
        levels = places.bit_length() - 1
        self.bits = [[b for b in range(levels) if b % 3 == d] for d in range(3)]
        self.y_per = max(1, 8 // self.span)
        self.z_per = max(1, 16 // self.span)
        self.x_shape = (2 * comps, self.span * 2, LANES)
        self.y_shape = (-(-2 // self.y_per) * comps, EDGE, LANES)
        self.z_shape = tile_shape(-(-self.half // self.z_per) * comps)
        self.x_count = len(self.bits[0])
        self.field = tile_shape(self.half, comps, self.span)
        self.slice = tile_shape(self.half, comps)
        self.messages = [self.x_shape] * self.x_count + [self.y_shape, self.z_shape, self.z_shape]
        self.z_ghost = pltpu.VMEM((2,) + self.z_shape, F32)


    def core(self):
        return lax.axis_index("tm") & 1

    def upper(self):
        return self.core() ^ (position(lax.axis_index("space"), self.bits[2]) & 1)

    def chip(self):
        return lax.axis_index("tm") >> 1

    def side(self, d):
        return 1 - (position(lax.axis_index("space"), self.bits[d]) & 1)


def position(place, bits):
    if len(bits) == 1:
        return place >> bits[0] & 1
    low, high = place >> bits[0] & 1, place >> bits[1] & 1
    return 2 * high + (low ^ high)


def exchange(sh, messages, n_time, places):
    axes = ("tm", "space")
    x_out, y_out, inner_out, z_out = messages[:-3], messages[-3], messages[-2], messages[-1]

    def pairs(bit, bits, halved):
        table = []
        for t in range(n_time):
            for s in range(places):
                here, there = position(s, bits), position(s ^ (1 << bit), bits)
                if abs(here - there) != 1:
                    continue
                if halved and (min(here, there) % 2 == 0) != (t % 2 == 1):
                    continue
                table.append((t * places + s, t * places + (s ^ (1 << bit))))
        return table

    z_in = lax.ppermute(z_out, axes, pairs(sh.bits[2][0], sh.bits[2], True))
    x_in = []
    for i, bit in enumerate(sh.bits[0]):
        x_in.append(lax.ppermute(x_out[i], axes, pairs(bit, sh.bits[0], False)))
    y_in = lax.ppermute(y_out, axes, pairs(sh.bits[1][0], sh.bits[1], False))
    inner_in = swap_cores(inner_out, n_time)
    return x_in + [y_in, inner_in, z_in]


def swap_cores(value, n_time):
    return lax.ppermute(value, "tm", [(t, t ^ 1) for t in range(n_time)])


def over_components(sh, visit):
    if sh.comps == 1:
        visit(0)
        return

    def step(comp, _):
        visit(comp)
        return 0

    lax.fori_loop(0, sh.comps, step, 0)


def over_tiles(sh, visit):
    def all_slots(comp):
        for j in range(sh.half):
            visit(j, comp)

    over_components(sh, all_slots)


def pack_faces(sh, tile, src, outs):
    on_top = sh.upper()
    lane = iota((EDGE, LANES), 1)
    within, group_of_lane = lane % EDGE, lane // EDGE
    x_outs, y_out, inner_out, z_out = outs[:-3], outs[-3], outs[-2], outs[-1]
    side_y = sh.side(1)

    def pack(comp):
        for g in range(-(-sh.half // sh.z_per)):
            low = [jnp.zeros((EDGE, LANES), F32)] * 2
            high = [jnp.zeros((EDGE, LANES), F32)] * 2
            for j in range(g * sh.z_per, min(sh.half, (g + 1) * sh.z_per)):
                for l in range(sh.span):
                    index = (j % sh.z_per) * sh.span + l
                    for h in range(2):
                        value = tile(j, comp, l, h)
                        value = pltpu.roll(value, index, 1) if index else value
                        low[h] = jnp.where(within == index, value, low[h])
                        high[h] = jnp.where(within == (index + EDGE - 1) % EDGE, value, high[h])
            for h in range(2):
                inner_out[g * sh.comps + comp, h] = jnp.where(on_top == 1, low[h], high[h])
                z_out[g * sh.comps + comp, h] = jnp.where(on_top == 1, high[h], low[h])
        for number, x_out in enumerate(x_outs):
            side = sh.side(0) if number == 0 else 1 - sh.side(0)
            for jj in range(2):
                for l in range(sh.span):
                    for h in range(2):
                        upper = src[2 * jj + 1, comp, l, h, EDGE - 1 : EDGE, :]
                        lower = src[2 * jj, comp, l, h, 0:1, :]
                        row = slice(2 * l + h, 2 * l + h + 1)
                        x_out[jj * sh.comps + comp, row, :] = jnp.where(side == 1, upper, lower)
        for y in range(-(-2 // sh.y_per)):
            packed = jnp.zeros((EDGE, LANES), F32)
            for jj in range(y * sh.y_per, min(2, (y + 1) * sh.y_per)):
                for l in range(sh.span):
                    index = (jj % sh.y_per) * sh.span + l
                    layer = src[2 * side_y + jj, comp, l, side_y]
                    layer = pltpu.roll(layer, EDGE * index, 1) if index else layer
                    packed = jnp.where(group_of_lane == (index + 7 * side_y) % 8, layer, packed)
            packed = jnp.where(side_y == 1, pltpu.roll(packed, EDGE, 1), packed)
            y_out[y * sh.comps + comp] = packed

    over_components(sh, pack)


def inner_sum(coef, src, j, comp, l):
    lane = iota((EDGE, LANES), 1)
    row = iota((EDGE, LANES), 0)
    tiles = [src[j, comp, l, h] for h in range(2)]
    if j // 2 == 0:
        below, above = 0.0, src[j ^ 2, comp, l, 0]
    else:
        below, above = src[j ^ 2, comp, l, 1], 0.0
    y_next = [jnp.where(lane < EDGE, tiles[1], tiles[0]), jnp.where(lane < EDGE, above, tiles[1])]
    last = lane >= LANES - EDGE
    y_back = [jnp.where(last, below, tiles[0]), jnp.where(last, tiles[0], tiles[1])]
    result = []
    for h in range(2):
        v = tiles[h]
        if j % 2 == 0:
            before, after = 0.0, src[j ^ 1, comp, l, h, 0:1, :]
        else:
            before, after = src[j ^ 1, comp, l, h, EDGE - 1 : EDGE, :], 0.0
        total = coef[j, YP, h] * pltpu.roll(y_next[h], LANES - EDGE, 1)
        total += coef[j, YM, h] * pltpu.roll(y_back[h], EDGE, 1)
        total += coef[j, ZP, h] * pltpu.roll(v, LANES - 1, 1)
        total += coef[j, ZM, h] * pltpu.roll(v, 1, 1)
        total += coef[j, XP, h] * pltpu.roll(jnp.where(row == 0, after, v), EDGE - 1, 0)
        total += coef[j, XM, h] * pltpu.roll(jnp.where(row == EDGE - 1, before, v), 1, 0)
        result.append(total)
    return result


def ghost_sum(sh, coef, faces, z_ghost, total, j, comp, l):
    xs, y_in = faces[:-1], faces[-1]
    x_side, x_row = j % 2, j // 2
    y_side, y_row = j // 2, j % 2
    y_index = (y_row % sh.y_per) * sh.span + l
    z_index = (j % sh.z_per) * sh.span + l
    z_group = (j // sh.z_per) * sh.comps + comp
    outer = x_row * sh.comps + comp
    result = []
    for h in range(2):
        value = total[h]
        value += coef[j, ZG, h] * pltpu.roll(
            z_ghost[z_index % 2, z_group, h], LANES - EDGE + 1 - z_index, 1
        )
        if h == y_side:
            group = y_in[(y_row // sh.y_per) * sh.comps + comp]
            shift = ((LANES - EDGE if y_side else 0) - EDGE * y_index) % LANES
            value += coef[j, YG, h] * (pltpu.roll(group, shift, 1) if shift else group)
        row = slice(2 * l + h, 2 * l + h + 1)
        if len(xs) == 1:
            crossed = xs[0][outer, row, :]
        else:
            wanted = sh.side(0) if x_side == 1 else 1 - sh.side(0)
            crossed = jnp.where(wanted == 1, xs[0][outer, row, :], xs[1][outer, row, :])
        part = slice(8 * x_side, 8 * x_side + 8)
        changed = value[part] + coef[j, XG, h, part, :] * jnp.broadcast_to(crossed, (8, LANES))
        parts = [value[:8], changed] if x_side else [changed, value[8:]]
        result.append(jnp.concatenate(parts, axis=0))
    return result


def place_z_ghost(sh, inner_in, z_in, z_ghost):
    upper = sh.upper()
    odd = iota((EDGE, LANES), 1) % 2 == 1

    def step(g, _):
        for h in range(2):
            inner, outer = inner_in[g, h], z_in[g, h]
            above = pltpu.roll(jnp.where(upper == 1, outer, inner), 2 * EDGE - 2, 1)
            below = jnp.where(upper == 1, inner, outer)
            z_ghost[0, g, h] = jnp.where(odd, below, above)
            z_ghost[1, g, h] = jnp.where(odd, above, below)
        return 0

    lax.fori_loop(0, inner_in.shape[0], step, 0)


def rows_to_tiles(read, count, rows, write):
    for chunk in range(CHUNKS):
        rows[chunk * count : (chunk + 1) * count, :] = read(chunk)
    for i in range(count):
        for h in range(2):
            write(i, h, rows[pl.ds(h * count + i, EDGE, 2 * count), :])


def tiles_to_rows(tile, count, rows, write):
    for i in range(count):
        for h in range(2):
            rows[pl.ds(h * count + i, EDGE, 2 * count), :] = tile(i, h)
    for chunk in range(CHUNKS):
        write(chunk, rows[chunk * count : (chunk + 1) * count, :])


def present(holder, slot, face):
    return jnp.where(holder[slot, face] >= 0, 1.0, 0.0).astype(F32)


def prepare_kernel(sh, *refs):
    far, (coef, first, own), rest = refs[:6], refs[6:9], refs[9:]
    near, (sems, rows, tiles, native_rows) = rest[:6], rest[6:]
    mine = pl.ds(sh.upper() * sh.half, sh.half)
    copies = [
        pltpu.make_async_copy(a.at[mine] if i == 5 else a, b, sems.at[i])
        for i, (a, b) in enumerate(zip(far, near))
    ]
    for copy in copies:
        copy.start()
    for copy in copies[:5]:
        copy.wait()
    coefficients(sh, *near[:5], coef, first, rows, tiles)
    copies[5].wait()
    unpack_half(sh, 0, near[5], own, 0, native_rows, 0)


def coefficients(sh, holder, mask, viscosity, peclet, initial, coef, first, rows, tiles):
    chip = sh.chip()
    slots = sh.slots

    def unpack(source, kind):
        def write(i, h, value):
            tiles[kind, i, h] = value

        rows_to_tiles(lambda c: source(c), slots, rows, write)

    unpack(lambda c: viscosity[:, c * LANES : (c + 1) * LANES], 0)
    for d in range(3):
        unpack(lambda c, d=d: peclet[d, :, c * LANES : (c + 1) * LANES], 1 + d)
    for d in range(3):
        unpack(lambda c, d=d: initial[d, :, c * LANES : (c + 1) * LANES], 4 + d)

    lane = iota((EDGE, LANES), 1)
    row = iota((EDGE, LANES), 0)
    within = lane % EDGE
    zero = jnp.zeros((EDGE, LANES), F32)

    def step(j, _):
        slot = sh.upper() * sh.half + j
        hold = [present(holder, slot, face) for face in range(FACES)]
        live = mask[slot].astype(F32)
        for h in range(2):
            nu = tiles[0, slot, h]
            inverse = 2.0 + 6.0 * nu
            q = 2.0 / inverse
            scale = nu / inverse
            plus = [scale * (1.0 - tiles[1 + d, slot, h]) for d in range(3)]
            minus = [scale * (1.0 + tiles[1 + d, slot, h]) for d in range(3)]
            for d, (upper, lower) in enumerate(((XP, XM), (YP, YM), (ZP, ZM))):
                coef[j, upper, h] = plus[d]
                coef[j, lower, h] = minus[d]
            coef[j, XP, h] = jnp.where(row < EDGE - 1, plus[0], plus[0] * hold[1])
            coef[j, XM, h] = jnp.where(row > 0, minus[0], minus[0] * hold[0])
            if h == 0:
                coef[j, YM, h] = jnp.where(lane >= EDGE, minus[1], minus[1] * hold[2])
            else:
                coef[j, YP, h] = jnp.where(lane < LANES - EDGE, plus[1], plus[1] * hold[3])
            coef[j, ZP, h] = jnp.where(within < EDGE - 1, plus[2], zero)
            coef[j, ZM, h] = jnp.where(within > 0, minus[2], zero)
            coef[j, XG, h] = jnp.where(
                row == 0,
                minus[0] * hold[0],
                jnp.where(row == EDGE - 1, plus[0] * hold[1], zero),
            )
            if h == 0:
                coef[j, YG, h] = jnp.where(lane < EDGE, minus[1] * hold[2], zero)
            else:
                coef[j, YG, h] = jnp.where(lane >= LANES - EDGE, plus[1] * hold[3], zero)
            coef[j, ZG, h] = jnp.where(
                within == 0,
                minus[2] * hold[4],
                jnp.where(within == EDGE - 1, plus[2] * hold[5], zero),
            )
            coef[j, Q, h] = q
            coef[j, INV, h] = inverse * live
            coef[j, LIVE, h] = jnp.zeros_like(nu) + live
            power = q
            for _ in range(sh.span.bit_length() - 1):
                power = power * power
            whole = power
            for _ in range(sh.chips.bit_length() - 1):
                whole = whole * whole
            weight = 1.0 / (1.0 - ALPHA_SCALE * whole)
            for back in range(1, sh.chips + 1):
                wrapped = jnp.where(chip < back, ALPHA_SCALE, 1.0)
                coef[j, K0 + back - 1, h] = weight * wrapped
                weight = weight * power
            for d in range(COMPONENTS):
                first[j, d, h] = tiles[4 + d, slot, h]
        return 0

    lax.fori_loop(0, sh.half, step, 0)


def unpack_half(sh, which, source, field, first, rows, base=None):
    def visit(j, comp):
        slot = (sh.upper() * sh.half if base is None else base) + j

        def read(c):
            return source[slot, comp, :, c * LANES : (c + 1) * LANES]

        def write(i, h, value):
            field[j, comp, first + i, h] = value

        rows_to_tiles(read, sh.local, rows.at[2 * j + which], write)

    over_tiles(sh, visit)


def gather_kernel(sh, own, other, field, last, *rest):
    core = sh.core()
    unpack_half(sh, 1, other, field, (1 - core) * sh.local, rest[-1])

    def visit(j, comp):
        for i in range(sh.local):
            for h in range(2):
                field[j, comp, core * sh.local + i, h] = own[j, comp, i, h]
        last[j, comp] = field[j, comp, sh.span - 1]

    over_tiles(sh, visit)
    pack_faces(sh, lambda j, c, l, h: field[j, c, l, h], field, rest[:-1])


def residual_inner_kernel(sh, coef, field, whole, other, inner, own_rows, other_rows, force, rows, sems):
    core = sh.core()
    mine = pl.ds(sh.upper() * sh.half, sh.half)
    copies = [
        pltpu.make_async_copy(source.at[mine], near, sems.at[i])
        for i, (source, near) in enumerate(((whole, own_rows), (other, other_rows)))
    ]
    for copy in copies:
        copy.start()

    def visit(j, comp):
        prior = None
        for l in range(sh.span):
            total = inner_sum(coef, field, j, comp, l)
            now = [field[j, comp, l, h] for h in range(2)]
            for h in range(2):
                value = total[h] - now[h]
                inner[j, comp, l, h] = value if prior is None else value + coef[j, Q, h] * prior[h]
            prior = now

    over_tiles(sh, visit)
    for copy in copies:
        copy.wait()
    unpack_half(sh, 0, own_rows, force, core * sh.local, rows, 0)
    unpack_half(sh, 1, other_rows, force, (1 - core) * sh.local, rows, 0)

    def add(j, comp):
        for l in range(sh.span):
            for h in range(2):
                inner[j, comp, l, h] += (0.5 * coef[j, Q, h]) * force[j, comp, l, h]

    over_tiles(sh, add)


def residual_outer_kernel(sh, coef, inner, before, first, *rest):
    faces = rest[: sh.x_count + 1]
    inner_in, z_in, scaled, partial, last, z_ghost = rest[sh.x_count + 1 :]
    place_z_ghost(sh, inner_in, z_in, z_ghost)
    chip = sh.chip()

    def visit(j, comp):
        carry = [jnp.zeros((EDGE, LANES), F32)] * 2
        for l in range(sh.span):
            total = [inner[j, comp, l, h] for h in range(2)]
            if l == 0:
                for h in range(2):
                    prior = jnp.where(chip == 0, first[j, sh.base + comp, h], before[j, comp, h])
                    total[h] = total[h] + coef[j, Q, h] * prior
            total = ghost_sum(sh, coef, faces, z_ghost, total, j, comp, l)
            for h in range(2):
                value = total[h] * coef[j, LIVE, h]
                scaled[j, comp, l, h] = value
                carry[h] = value + coef[j, Q, h] * carry[h]
                partial[j, comp, l, h] = carry[h]
        for h in range(2):
            last[j, comp, h] = carry[h]

    over_tiles(sh, visit)


def sweep_inner_kernel(sh, coef, field, scaled, inner):
    def visit(j, comp):
        for l in range(sh.span):
            total = inner_sum(coef, field, j, comp, l)
            for h in range(2):
                inner[j, comp, l, h] = scaled[j, comp, l, h] + total[h]

    over_tiles(sh, visit)


def sweep_outer_kernel(sh, coef, inner, *rest):
    faces = rest[: sh.x_count + 1]
    inner_in, z_in, partial, last, z_ghost = rest[sh.x_count + 1 :]
    place_z_ghost(sh, inner_in, z_in, z_ghost)

    def visit(j, comp):
        carry = [jnp.zeros((EDGE, LANES), F32)] * 2
        for l in range(sh.span):
            total = [inner[j, comp, l, h] for h in range(2)]
            total = ghost_sum(sh, coef, faces, z_ghost, total, j, comp, l)
            for h in range(2):
                carry[h] = total[h] + coef[j, Q, h] * carry[h]
                partial[j, comp, l, h] = carry[h]
        for h in range(2):
            last[j, comp, h] = carry[h]

    over_tiles(sh, visit)


def incoming_slice(sh, coef, lasts, j, comp, h):
    total = coef[j, K0, h] * lasts[0][j, comp, h]
    for back in range(1, sh.chips):
        total += coef[j, K0 + back, h] * lasts[back][j, comp, h]
    return total


def close_kernel(sh, coef, partial, *rest):
    lasts, (field, *messages) = rest[: sh.chips], rest[sh.chips :]
    term = {}

    def tile(j, comp, l, h):
        if l == 0:
            term[h] = incoming_slice(sh, coef, lasts, j, comp, h)
        term[h] = coef[j, Q, h] * term[h]
        value = partial[j, comp, l, h] + term[h]
        field[j, comp, l, h] = value
        return value

    pack_faces(sh, tile, field, messages)


def velocity_kernel(sh, whole, other, field, out, send, rows, kept, sems):
    core = sh.core()
    own, others = core * sh.local, (1 - core) * sh.local

    def visit(j, comp):
        slot = sh.upper() * sh.half + j

        def keep(c, value):
            at = slice(c * LANES, (c + 1) * LANES)
            kept[j, comp, :, at] = whole[slot, comp, :, at] + value

        def pass_on(c, value):
            at = slice(c * LANES, (c + 1) * LANES)
            send[j, comp, :, at] = other[slot, comp, :, at] + value

        tiles_to_rows(lambda i, h: field[j, comp, own + i, h], sh.local, rows.at[2 * j], keep)
        tiles_to_rows(
            lambda i, h: field[j, comp, others + i, h], sh.local, rows.at[2 * j + 1], pass_on
        )

    def component(comp):
        for j in range(sh.half):
            visit(j, comp)
        put_copy(sh, comp, kept, out, sems).start()

    over_components(sh, component)
    wait_copies(sh, kept, out, sems)


def put_copy(sh, comp, kept, out, sems):
    slots = pl.ds(sh.upper() * sh.half, sh.half)
    return pltpu.make_async_copy(kept.at[:, comp], out.at[slots, comp], sems.at[comp])


def wait_copies(sh, kept, out, sems):
    for comp in range(sh.comps):
        put_copy(sh, comp, kept, out, sems).wait()


def bounce_copies(sh, comp, half, out, buffer, sems):
    slots = pl.ds((1 - sh.upper()) * sh.half, sh.half)
    first = pltpu.make_async_copy(half.at[:, comp], buffer.at[:, comp], sems.at[0, comp])
    if out is None:
        return first, None
    return first, pltpu.make_async_copy(
        buffer.at[:, comp], out.at[slots, comp], sems.at[1, comp]
    )


def start_bounce(sh, half, buffer, sems):
    for comp in range(sh.comps):
        bounce_copies(sh, comp, half, None, buffer, sems)[0].start()


def end_bounce(sh, half, out, buffer, sems):
    for comp in range(sh.comps):
        first, second = bounce_copies(sh, comp, half, out, buffer, sems)
        first.wait()
        second.start()
    for comp in range(sh.comps):
        bounce_copies(sh, comp, half, out, buffer, sems)[1].wait()


def place_kernel(sh, half, partial, out, buffer, sems):
    start_bounce(sh, half, buffer, sems)
    end_bounce(sh, half, out, buffer, sems)


def final_inner_kernel(sh, coef, field, scaled, *rest):
    lasts, (inner,) = rest[: sh.chips], rest[sh.chips :]
    chip = sh.chip()

    def visit(j, comp):
        prior = [
            jnp.where(chip == 0, 0.0, incoming_slice(sh, coef, lasts, j, comp, h))
            for h in range(2)
        ]
        for l in range(sh.span):
            total = inner_sum(coef, field, j, comp, l)
            for h in range(2):
                now = field[j, comp, l, h]
                value = scaled[j, comp, l, h] + total[h] - now
                inner[j, comp, l, h] = value + coef[j, Q, h] * prior[h]
                prior[h] = now

    over_tiles(sh, visit)


def final_outer_kernel(sh, mine, coef, inner, *rest):
    faces = rest[: sh.x_count + 1]
    if mine:
        inner_in, z_in, half, partial, out, placed, z_ghost, hold, rows, *kept = rest[sh.x_count + 1 :]
        bounce = kept[2:]
        start_bounce(sh, half, *bounce)
    else:
        inner_in, z_in, out, z_ghost, hold, rows = rest[sh.x_count + 1 :]
    target = kept[0] if mine else out
    place_z_ghost(sh, inner_in, z_in, z_ghost)
    core = sh.core()

    for number in range(2):

        def visit(j, comp, number=number):
            for i in range(sh.local):
                l = number * sh.local + i
                total = [inner[j, comp, l, h] for h in range(2)]
                total = ghost_sum(sh, coef, faces, z_ghost, total, j, comp, l)
                for h in range(2):
                    hold[j, i, h] = total[h] * coef[j, INV, h]

            def write(c, value):
                target[j, comp, :, c * LANES : (c + 1) * LANES] = value

            tiles_to_rows(lambda i, h: hold[j, i, h], sh.local, rows.at[j], write)

        def component(comp, visit=visit):
            for j in range(sh.half):
                visit(j, comp)
            if mine:
                put_copy(sh, comp, kept[0], out, kept[1]).start()

        @pl.when(core == (number if mine else 1 - number))
        def _(component=component):
            over_components(sh, component)

    if mine:
        end_bounce(sh, half, placed, *bounce)
        wait_copies(sh, kept[0], out, kept[1])


def bind(kernel, sh, *fixed):
    def run(*refs):
        kernel(sh, *fixed, *refs)

    return run


def body(
    iterate,
    forcing,
    initial_velocity,
    viscosity,
    peclet,
    live_patch_mask,
    neighbour_holder,
    neighbour_slot,
):
    n_time, places = lax.axis_size("tm"), lax.axis_size("space")
    slots, local = iterate.shape[:2]
    shapes = [Shape(slots, local, n_time, places, base, comps) for base, comps in STREAMS]
    sh = shapes[0]
    half = sh.half
    velocity = iterate.transpose(0, 2, 1, 3)
    force = forcing.transpose(0, 2, 1, 3)

    velocity_other = swap_cores(velocity, n_time)
    force_other = swap_cores(force, n_time)

    rows = pltpu.VMEM((2 * half, CHUNKS * local, LANES), F32)

    native = (half, COMPONENTS, local, CHUNKS * LANES)
    whole = (slots,) + native[1:]
    params = [
        neighbour_holder,
        live_patch_mask,
        viscosity,
        peclet.transpose(1, 0, 2),
        initial_velocity.transpose(1, 0, 2),
    ]
    near = [(pltpu.SMEM if i < 2 else pltpu.VMEM)(p.shape, p.dtype) for i, p in enumerate(params)]
    sh = shapes[0]
    coef, first, own = call(
        bind(prepare_kernel, sh),
        params + [velocity],
        [tile_shape(half, K0 + sh.chips), tile_shape(half, COMPONENTS), tile_shape(half, COMPONENTS, local)],
        near
        + [
            pltpu.VMEM(native, F32),
            pltpu.SemaphoreType.DMA((6,)),
            pltpu.VMEM((CHUNKS * slots, LANES), F32),
            pltpu.VMEM(tile_shape(7, slots), F32),
            rows,
        ],
        flops=WORK,
        far=range(6),
        grant=GRANT - velocity.size * 4 * 9 // 4,
    )
    coef, first, own, arrived = lax.optimization_barrier((coef, first, own, velocity_other))
    fields, faces, befores = [], [], []
    for sh in shapes:
        field, last, *out = call(
            bind(gather_kernel, sh), [own, arrived], [sh.field, sh.slice] + sh.messages, [rows]
        )
        befores.append(lax.ppermute(last, "tm", [(a, (a + 2) % n_time) for a in range(n_time)]))
        faces.append(exchange(sh, out, n_time, places))
        fields.append(field)

    def chip_ends(sh, last):
        return [
            lax.ppermute(last, "tm", [(a, (a + 2 * back) % n_time) for a in range(n_time)])
            for back in range(1, sh.chips)
        ] + [last]

    scaleds, partials, ends = [], [], []
    for sh, field, before, face in zip(shapes, fields, befores, faces):
        (inner,) = call(
            bind(residual_inner_kernel, sh),
            [coef, field, force, force_other],
            [sh.field],
            [pltpu.VMEM(native, F32)] * 2
            + [pltpu.VMEM(sh.field, F32), rows, pltpu.SemaphoreType.DMA((2,))],
            flops=sh.comps * WORK,
            far=(2, 3),
        )
        scaled, partial, last = call(
            bind(residual_outer_kernel, sh),
            [coef, inner, before, first] + face,
            [sh.field, sh.field, sh.slice],
            [sh.z_ghost],
            flops=sh.comps * WORK,
        )
        scaleds.append(scaled)
        partials.append(partial)
        ends.append(chip_ends(sh, last))

    corrections = [None] * len(shapes)
    for sweep in range(SWEEPS):
        for number, sh in enumerate(shapes):
            if sweep > 0:
                (inner,) = call(
                    bind(sweep_inner_kernel, sh),
                    [coef, corrections[number], scaleds[number]],
                    [sh.field],
                    flops=sh.comps * WORK,
                )
                partials[number], last = call(
                    bind(sweep_outer_kernel, sh),
                    [coef, inner] + faces[number],
                    [sh.field, sh.slice],
                    [sh.z_ghost],
                    flops=sh.comps * WORK,
                )
                ends[number] = chip_ends(sh, last)
            corrections[number], *out = call(
                bind(close_kernel, sh),
                [coef, partials[number]] + ends[number],
                [sh.field] + sh.messages,
                flops=sh.comps * WORK,
            )
            faces[number] = exchange(sh, out, n_time, places)
    sh = shapes[0]
    (inner,) = call(
        bind(final_inner_kernel, sh),
        [coef, corrections[0], scaleds[0]] + ends[0],
        [sh.field],
        flops=sh.comps * WORK,
    )
    held_back, inner = lax.optimization_barrier((corrections[0], inner))
    copied = [pltpu.VMEM(native, F32), pltpu.SemaphoreType.DMA((COMPONENTS,))]
    bounce = [pltpu.VMEM(native, F32), pltpu.SemaphoreType.DMA((2, COMPONENTS))]
    velocity_out, send = call(
        bind(velocity_kernel, sh),
        [velocity, velocity_other, held_back],
        [whole, native],
        [rows] + copied,
        flops=WORK,
        far_outs=(0,),
    )
    velocity_other = swap_cores(send, n_time)
    (send,) = call(
        bind(final_outer_kernel, sh, False),
        [coef, inner] + faces[0],
        [native],
        [sh.z_ghost, pltpu.VMEM(tile_shape(half, local), F32), rows],
        flops=WORK,
    )
    residual_other = swap_cores(send, n_time)
    ins = [coef, inner] + faces[0] + [velocity_other, velocity_out]
    residual_out, corrected_velocity = call(
        bind(final_outer_kernel, sh, True),
        ins,
        [whole, whole],
        [sh.z_ghost, pltpu.VMEM(tile_shape(half, local), F32), rows] + copied + bounce,
        flops=WORK,
        far=(len(ins) - 2, len(ins) - 1),
        far_outs=(0, 1),
        alias={len(ins) - 1: 1},
    )
    (corrected_residual,) = call(
        bind(place_kernel, sh),
        [residual_other, residual_out],
        [whole],
        bounce,
        far=(0, 1),
        far_outs=(0,),
        alias={1: 0},
    )
    return corrected_velocity.transpose(0, 2, 1, 3), corrected_residual.transpose(0, 2, 1, 3)


def solution(mesh):
    return jax.shard_map(
        body,
        mesh=mesh,
        in_specs=(
            P("space", "tm", None, None),
            P("space", "tm", None, None),
            P("space", None, None),
            P("space", None),
            P("space", None, None),
            P("space"),
            P("space", None),
            P("space", None),
        ),
        out_specs=(P("space", "tm", None, None), P("space", "tm", None, None)),
        check_vma=False,
    )
```
